256 devices in a mesh: row: 16 (over z, x_lo), col: 16 (over x_hi, y, core).
Axes of the slice: x: 4 (x_hi: 2, x_lo: 2; x = x_hi * 2 + x_lo), y: 4, z: 8, core: 2. Of those that a mesh axis runs over, the one named last changes fastest.
Arguments:
- gradients: bfloat16 [16, 16, 4, 64, 1536], P('row', 'col'), may hold values from -96 to 96
- token_counts: int32 [16, 16], P('row', 'col'), may hold values from 16 to 256
- row_groups: int32 [2, 16, 16], replicated, may hold values from 0 to 15, each once within a row
- col_groups: int32 [1, 16, 16], replicated, may hold values from 0 to 15, each once within a row
Outputs:
- averaged: float32 [16, 16, 4, 64, 1536], P('row', 'col')
- totals: int32 [16, 16], P('row', 'col')
The draws below stay inside these ranges and needn't reach their ends.
Inputs may be any that keep to these rules, and one draw needn't show every extreme that they name: row_groups[r, i] lists the 16 grid columns in some order: in row round r, grid row i's member of group g sits in column row_groups[r, i, g]. col_groups[0, j] lists the 16 grid rows in some order: grid column j's member of group h sits in row col_groups[0, j, h].
All inputs are finite; a program needn't handle non-finite values.
Results may differ from the reference program's by a relative error of at most 0.0003.
Values may be sent and summed in bfloat16 or wider, within the bound.
A program may use at most 64 MiB of HBM per device.

```python
import jax
import jax.numpy as jnp

D = 1536
BLOCKS = 4
GR = 64
N_ROW = 16
N_COL = 16


def with_ends(drawn, rng, smallest, largest):
    spot = [jax.random.randint(jax.random.fold_in(rng, axis), (), 0, length) for axis, length in enumerate(drawn.shape)]
    widest = drawn.shape.index(max(drawn.shape))
    beside = spot[:widest] + [(spot[widest] + 1) % drawn.shape[widest]] + spot[widest + 1:]
    return drawn.at[tuple(spot)].set(smallest).at[tuple(beside)].set(largest)


def block_scale(rng, dims, split, smallest, high):
    def one(dim, blocks):
        steps = jax.random.uniform(jax.random.fold_in(jax.random.fold_in(rng, 6), dim), (blocks,), jnp.float32, smallest / len(split), high / len(split))
        return jnp.repeat(jnp.exp(steps), dims[dim] // blocks).reshape((-1,) + (1,) * (len(dims) - dim - 1))

    level = one(*split[0])
    for cut in split[1:]:
        level = level * one(*cut)
    return level


def centred(rng, extent, deviation, reach, pieces=(), dtype=jnp.bfloat16):
    array = deviation * jax.random.normal(rng, extent, jnp.float32)
    if pieces:
        array = array * block_scale(rng, extent, pieces, -0.22, 0.18)
    return jnp.clip(array, -reach, reach).astype(dtype)


def setup_inputs(seed: int = 0) -> dict:
    seeds = jax.random.split(jax.random.key(seed), 5)
    return {
        "gradients": centred(seeds[0], (N_ROW, N_COL, BLOCKS, GR, D), 16.0, 96.0, ((0, 16), (1, 16))),
        "token_counts": with_ends(jax.random.randint(seeds[1], (N_ROW, N_COL), 16, 257), jax.random.fold_in(seeds[1], 1), 16, 256).astype(jnp.int32),
        "row_groups": jax.vmap(lambda own: jax.random.permutation(own, N_COL))(jax.random.split(seeds[2], 2 * N_ROW)).reshape((2, N_ROW, N_COL)).astype(jnp.int32),
        "col_groups": jax.vmap(lambda own: jax.random.permutation(own, N_ROW))(jax.random.split(seeds[3], 1 * N_COL)).reshape((1, N_COL, N_ROW)).astype(jnp.int32),
    }


def groups_average(values, weights, group_order):
    picked = jnp.take_along_axis(values, group_order[:, :, None, None], axis=1)
    picked_w = jnp.take_along_axis(weights, group_order, axis=1)
    group_sums = jnp.sum(picked * picked_w[:, :, None, None], axis=0)
    group_totals = jnp.sum(picked_w, axis=0)
    averaged = group_sums / group_totals[:, None, None]
    inverse = jnp.argsort(group_order, axis=1).astype(jnp.int32)
    return averaged[inverse], group_totals[inverse]


def reference(gradients, token_counts, row_groups, col_groups):
    grad_state = gradients.reshape(N_ROW, N_COL, BLOCKS * GR, D).astype(jnp.float32)
    weight = token_counts.astype(jnp.float32)
    grad_state, weight = groups_average(grad_state, weight, row_groups[0])
    swapped, swapped_w = groups_average(jnp.swapaxes(grad_state, 0, 1), weight.T, col_groups[0])
    grad_state = jnp.swapaxes(swapped, 0, 1)
    weight = swapped_w.T
    grad_state, weight = groups_average(grad_state, weight, row_groups[1])
    return grad_state.reshape(gradients.shape), weight.astype(jnp.int32)
```

```python
import jax
import jax.numpy as jnp
from jax import lax
from jax.experimental import pallas as pl
from jax.experimental.pallas import tpu as pltpu
from jax.sharding import PartitionSpec as P

MESH = pl.DeviceIdType.MESH
NZ = 8
NPLANE = 32
NG = 16
ROWS = 16
LANES = 768
PIECES = 3
L = LANES // PIECES
OCTAVES = 24.0
TOP = 32767.0
TINY = 1.2e-38

PLANE = [(dx, dy, dc) for dx in range(4) for dy in range(4) for dc in range(2) if (dx, dy, dc) != (0, 0, 0)]
ZS = (1, 7, 2, 6, 3, 5, 4)


def iota(shape, dim):
    return lax.broadcasted_iota(jnp.int32, shape, dim)


def onehot(cond):
    return jnp.where(cond, 1.0, 0.0).astype(jnp.bfloat16)


def mm(a, b):
    return jnp.dot(a, b, preferred_element_type=jnp.float32)


def mm_nt(a, b):
    return lax.dot_general(a, b, (((1,), (1,)), ((), ())), preferred_element_type=jnp.float32)


def small(ints):
    return ints.astype(jnp.float32).astype(jnp.bfloat16)


def body(
    grad, count, rg, cg, codes, info,
    gv, mine, metas, zmine, zmetas, took, base, pick, spread, blend, part, ring, full, chosen,
    load_sem, own_sem, meta_s, meta_r, zmeta_s, zmeta_r, a_s, a_r, up_s, up_r, dn_s, dn_r, g_s, g_r, b_s, b_r,
):
    row, col = lax.axis_index("row"), lax.axis_index("col")
    z, xl = row // 2, row % 2
    xh, y, c = col // 8, (col // 2) % 4, col % 2
    x = 2 * xh + xl
    q = xl * 16 + col

    def plane_peer(off):
        px, py, pc = (x + off[0]) % 4, (y + off[1]) % 4, (c + off[2]) % 2
        pcol = ((px // 2) * 4 + py) * 2 + pc
        return (2 * z + px % 2, pcol), (px % 2) * 16 + pcol

    def z_peer(dz):
        return (2 * ((z + dz) % NZ) + xl, col)

    def spot(which):
        return pl.multiple_of((which // 2) * ROWS, ROWS), (which % 2) * LANES

    def piece_of(which, p):
        r0, l0 = spot(which)
        return pl.ds(r0, ROWS), pl.ds(pl.multiple_of(l0 + p * L, 128), L)

    peers = [plane_peer(off) for off in PLANE]

    load = pltpu.make_async_copy(grad, gv, load_sem)
    load.start()
    owns = []
    for p in range(PIECES):
        rs, ls = piece_of(q, p)
        own = pltpu.make_async_copy(grad.at[rs, ls], took.at[p, pl.ds(pl.multiple_of(q * ROWS, ROWS), ROWS)], own_sem.at[p])
        own.start()
        owns.append(own)

    barrier = pltpu.get_barrier_semaphore()
    for dev, _ in peers:
        pl.semaphore_signal(barrier, inc=1, device_id=dev, device_id_type=MESH)
    for dz in ZS:
        pl.semaphore_signal(barrier, inc=1, device_id=z_peer(dz), device_id_type=MESH)

    load.wait()
    largest = jnp.max(jnp.abs(gv[...].astype(jnp.float32)))
    own_w = count[0, 0].astype(jnp.float32)
    mine[...] = jnp.where(iota((1, 128), 1) < 64, own_w, largest)

    pl.semaphore_wait(barrier, len(PLANE) + len(ZS))

    waits = []
    meta_bytes = metas.at[pl.ds(0, len(PLANE))]
    for dev, _ in peers:
        pltpu.make_async_remote_copy(
            src_ref=mine, dst_ref=metas.at[q], send_sem=meta_s, recv_sem=meta_r, device_id=dev, device_id_type=MESH
        ).start()
    for p in range(PIECES):
        for dev, pq in peers:
            rs, ls = piece_of(pq, p)
            pltpu.make_async_remote_copy(
                src_ref=gv.at[rs, ls],
                dst_ref=took.at[p, pl.ds(pl.multiple_of(q * ROWS, ROWS), ROWS)],
                send_sem=a_s.at[p], recv_sem=a_r.at[p], device_id=dev, device_id_type=MESH,
            ).start()
    metas[q] = mine[...]

    rg0, rg1, cg0 = small(rg[0]), small(rg[1]), small(cg[0])
    eye = onehot(iota((NG, NG), 0) == iota((NG, NG), 1))
    by_i = onehot(iota((256, NG), 0) // 16 == iota((256, NG), 1))
    j_of = (iota((256, NG), 0) % 16).astype(jnp.float32)
    first = onehot(mm(by_i, rg0) == j_of)
    last = onehot(mm(by_i, rg1) == j_of)
    n_i = onehot(iota((NG, 256), 1) // 16 == iota((NG, 256), 0))
    n_j = onehot(iota((NG, 256), 1) % 16 == iota((NG, 256), 0))
    cols_t = mm_nt(eye, cg0).astype(jnp.bfloat16)
    rows_t = mm_nt(eye, rg1).astype(jnp.bfloat16)
    middle = onehot(mm(cols_t, n_j) == (iota((NG, 256), 1) // 16).astype(jnp.float32))
    third = onehot(mm(rows_t, n_i) == (iota((NG, 256), 1) % 16).astype(jnp.float32))
    m2 = mm(middle, first).astype(jnp.bfloat16)
    m3 = mm_nt(third, middle).astype(jnp.bfloat16)
    m = mm(m3, m2)
    mb = m.astype(jnp.bfloat16)

    in_plane = onehot(iota((NPLANE, 256), 1) == iota((NPLANE, 256), 0) + 32 * z)
    first_z = mm(in_plane, first).astype(jnp.bfloat16)
    last_z = mm(in_plane, last).astype(jnp.bfloat16)
    row_g = onehot(iota((256, NG), 0) % 16 == iota((256, NG), 1))
    col_q = onehot(iota((NPLANE, 512), 1) // 16 == iota((NPLANE, 512), 0))
    wide = mm(mm_nt(row_g, first_z).astype(jnp.bfloat16), col_q)
    base[...] = jnp.where(iota((256, 512), 0) // 16 == iota((256, 512), 1) % 16, wide, 0.0)
    row_q = onehot(iota((512, NPLANE), 0) // 16 == iota((512, NPLANE), 1))
    col_k = onehot(iota((NG, 256), 1) % 16 == iota((NG, 256), 0))
    tall = mm(mm(row_q, last_z).astype(jnp.bfloat16), col_k)
    pick[...] = jnp.where(iota((512, 256), 0) % 16 == iota((512, 256), 1) // 16, tall, 0.0).astype(jnp.bfloat16)

    r32 = onehot(iota((32, NG), 0) % 16 == iota((32, NG), 1))
    c96 = onehot(iota((NG, 96), 1) % 16 == iota((NG, 96), 0))
    mix = mm(mm(r32, mb).astype(jnp.bfloat16), c96)
    blend[...] = jnp.where(iota((32, 96), 0) // 16 == (iota((32, 96), 1) // 16) % 2, mix, 0.0).astype(jnp.bfloat16)

    pltpu.make_async_copy(meta_bytes, meta_bytes, meta_r).wait()
    held = metas[:, 0, :]
    lane = iota((NPLANE, 128), 1)
    plane_w = jnp.sum(jnp.where(lane == iota((NPLANE, 128), 0), held[:, 0:1], 0.0), axis=0, keepdims=True)
    plane_x = jnp.max(jnp.where(lane >= 64, held, 0.0))
    zmine[...] = jnp.where(iota((1, 128), 1) < NPLANE, plane_w, plane_x)
    for dz in ZS:
        pltpu.make_async_remote_copy(
            src_ref=zmine, dst_ref=zmetas.at[z], send_sem=zmeta_s, recv_sem=zmeta_r, device_id=z_peer(dz), device_id_type=MESH
        ).start()
    zmetas[z] = zmine[...]
    w512 = mm(plane_w[:, 0:NPLANE].astype(jnp.bfloat16), col_q)
    spread[...] = (base[...] * w512).astype(jnp.bfloat16)

    def z_copy(p, up, step, src):
        s_sem, r_sem = (up_s, up_r) if up else (dn_s, dn_r)
        return pltpu.make_async_remote_copy(
            src_ref=src, dst_ref=ring.at[p, 0 if up else 1, step], send_sem=s_sem.at[p, step], recv_sem=r_sem.at[p, step],
            device_id=z_peer(1 if up else 7), device_id_type=MESH,
        )

    def chunk(dz):
        return pl.ds(pl.multiple_of(((z + dz) % NZ) * 32, 32), 32)

    def hops(p, up):
        return 4 if up == (p % 2 == 0) else 3

    sent = []

    def open_piece(p):
        owns[p].wait()
        got = took.at[p, pl.ds(0, len(PLANE) * ROWS)]
        pltpu.make_async_copy(got, got, a_r.at[p]).wait()
        part[p] = mm(spread[...], took[p])
        for up in (True, False):
            far = hops(p, up)
            cp = z_copy(p, up, 0, part.at[p, chunk(far if up else -far)])
            cp.start()
            sent.append(cp)

    def ring_step(p, step):
        for up in (True, False):
            far = hops(p, up)
            if step >= far:
                continue
            z_copy(p, up, step - 1, part.at[p, chunk(0)]).wait_recv()
            away = far - step
            slot = ring.at[p, 0 if up else 1, step - 1]
            slot[...] = slot[...] + part[p, chunk(away if up else -away), :]
            cp = z_copy(p, up, step, slot)
            cp.start()
            sent.append(cp)

    ztot = {}

    def totals_now():
        got = zmetas.at[pl.ds(0, NZ - 1)]
        pltpu.make_async_copy(got, got, zmeta_r).wait()
        cw = zmetas[:, 0, :]
        by_z = onehot(iota((256, NZ), 0) // 32 == iota((256, NZ), 1))
        lanes = iota((256, 128), 1)
        all_x = jnp.maximum(jnp.max(jnp.where(iota((NZ, 128), 1) >= NPLANE, cw, 0.0)), TINY)
        counts = jnp.where(iota((NZ, 128), 1) < NPLANE, cw, 0.0).astype(jnp.bfloat16)
        spread_w = mm(by_z, counts)
        w_col = jnp.sum(jnp.where(lanes == iota((256, 128), 0) % 32, spread_w, 0.0), axis=1, keepdims=True)
        c1 = jnp.sum(first.astype(jnp.float32) * w_col, axis=0, keepdims=True)
        c3 = jnp.sum(m * c1, axis=1, keepdims=True)
        ztot["x"] = all_x
        ztot["c3"] = jnp.concatenate([c3, c3], axis=0)
        is_me = onehot(iota((NG, NPLANE), 1) == q)
        mine_k = mm(is_me, last_z)
        own_c3 = jnp.sum(jnp.where(iota((NG, NG), 0) == iota((NG, NG), 1), mine_k, 0.0) * c3)
        info[...] = jnp.where(iota((8, 128), 1) < 64, own_c3, all_x)

    def mix_piece(p):
        for up in (True, False):
            z_copy(p, up, hops(p, up) - 1, part.at[p, chunk(0)]).wait_recv()
        total = part[p, chunk(0), :] + ring[p, 0, hops(p, True) - 1] + ring[p, 1, hops(p, False) - 1]
        hi = total.astype(jnp.bfloat16)
        rest = total - hi.astype(jnp.float32)
        mid = rest.astype(jnp.bfloat16)
        low = (rest - mid.astype(jnp.float32)).astype(jnp.bfloat16)
        mixed = mm(blend[...], jnp.concatenate([hi, mid, low], axis=0))
        avg = mixed / ztot["c3"]
        size = jnp.abs(avg) * (1.0 / ztot["x"])
        level = TOP + jnp.log2(jnp.maximum(size, 1e-30)) * (TOP / OCTAVES)
        level = jnp.clip(jnp.round(level), 0.0, TOP)
        full[p, chunk(0), :] = jnp.where(avg < 0, -level, level).astype(jnp.int32).astype(jnp.int16)
        for dz in ZS:
            pltpu.make_async_remote_copy(
                src_ref=full.at[p, chunk(0)], dst_ref=full.at[p, chunk(0)], send_sem=g_s.at[p], recv_sem=g_r.at[p],
                device_id=z_peer(dz), device_id_type=MESH,
            ).start()

    def send_piece(p):
        got = full.at[p, pl.ds(0, (NZ - 1) * 32)]
        pltpu.make_async_copy(got, got, g_r.at[p]).wait()
        code = full[p].astype(jnp.int32)
        high = code >> 8
        lows = code & 255
        high_sel = mm(pick[...], small(high))
        low_sel = mm(pick[...], small(lows))
        chosen[p] = (high_sel * 256.0 + low_sel).astype(jnp.int32).astype(jnp.int16)
        rs, ls = piece_of(q, p)
        for dev, pq in peers:
            pltpu.make_async_remote_copy(
                src_ref=chosen.at[p, pl.ds(pl.multiple_of(pq * ROWS, ROWS), ROWS)], dst_ref=codes.at[rs, ls],
                send_sem=b_s.at[p], recv_sem=b_r.at[p], device_id=dev, device_id_type=MESH,
            ).start()
        codes[rs, ls] = chosen[p, pl.ds(pl.multiple_of(q * ROWS, ROWS), ROWS), :]

    for t in range(PIECES + 6):
        for p in range(PIECES):
            step = t - p
            if 1 <= step <= 3:
                ring_step(p, step)
            elif step == 4:
                if p == 0:
                    totals_now()
                mix_piece(p)
            elif step == 6:
                send_piece(p)
        if t < PIECES:
            open_piece(t)

    for p in range(PIECES):
        got = chosen.at[p, pl.ds(0, len(PLANE) * ROWS)]
        pltpu.make_async_copy(got, got, b_r.at[p]).wait()
    pltpu.make_async_copy(meta_bytes, meta_bytes, meta_s).wait()
    zm = zmetas.at[pl.ds(0, NZ - 1)]
    pltpu.make_async_copy(zm, zm, zmeta_s).wait()
    for cp in sent:
        cp.wait_send()
    for p in range(PIECES):
        a = took.at[p, pl.ds(0, len(PLANE) * ROWS)]
        pltpu.make_async_copy(a, a, a_s.at[p]).wait()
        g = full.at[p, pl.ds(0, (NZ - 1) * 32)]
        pltpu.make_async_copy(g, g, g_s.at[p]).wait()
        b = chosen.at[p, pl.ds(0, len(PLANE) * ROWS)]
        pltpu.make_async_copy(b, b, b_s.at[p]).wait()


def local(gradients, token_counts, row_groups, col_groups):
    flat = gradients.reshape(ROWS * 16, 2 * LANES)
    dma = pltpu.SemaphoreType.DMA
    vmem = pl.BlockSpec(memory_space=pltpu.VMEM)
    codes, info = pl.pallas_call(
        body,
        out_shape=(
            jax.ShapeDtypeStruct((256, 2 * LANES), jnp.int16),
            jax.ShapeDtypeStruct((8, 128), jnp.float32),
        ),
        in_specs=[pl.BlockSpec(memory_space=pl.ANY), pl.BlockSpec(memory_space=pltpu.SMEM), vmem, vmem],
        out_specs=(vmem, vmem),
        scratch_shapes=[
            pltpu.VMEM((256, 2 * LANES), jnp.bfloat16),
            pltpu.VMEM((1, 128), jnp.float32),
            pltpu.VMEM((NPLANE, 1, 128), jnp.float32),
            pltpu.VMEM((1, 128), jnp.float32),
            pltpu.VMEM((NZ, 1, 128), jnp.float32),
            pltpu.VMEM((PIECES, 512, L), jnp.bfloat16),
            pltpu.VMEM((256, 512), jnp.float32),
            pltpu.VMEM((512, 256), jnp.bfloat16),
            pltpu.VMEM((256, 512), jnp.bfloat16),
            pltpu.VMEM((32, 96), jnp.bfloat16),
            pltpu.VMEM((PIECES, 256, L), jnp.float32),
            pltpu.VMEM((PIECES, 2, 4, 32, L), jnp.float32),
            pltpu.VMEM((PIECES, 256, L), jnp.int16),
            pltpu.VMEM((PIECES, 512, L), jnp.int16),
            dma, dma((PIECES,)), dma, dma, dma, dma,
            dma((PIECES,)), dma((PIECES,)),
            dma((PIECES, 4)), dma((PIECES, 4)), dma((PIECES, 4)), dma((PIECES, 4)),
            dma((PIECES,)), dma((PIECES,)), dma((PIECES,)), dma((PIECES,)),
        ],
        compiler_params=pltpu.CompilerParams(collective_id=0, has_side_effects=True),
        name="group_average",
    )(flat, token_counts, row_groups, col_groups)
    number = codes.astype(jnp.int32)
    level = jnp.abs(number).astype(jnp.float32)
    size = info[0, 127] * jnp.exp2((level - TOP) * (OCTAVES / TOP))
    averaged = jnp.where(number == 0, 0.0, jnp.where(number < 0, -size, size))
    return averaged.reshape(gradients.shape), info[0, 0].astype(jnp.int32).reshape(token_counts.shape)


def solution(mesh):
    placed = (P("row", "col", None, None, None), P("row", "col"), P(), P())
    return jax.shard_map(
        local,
        mesh=mesh,
        in_specs=placed,
        out_specs=(P("row", "col", None, None, None), P("row", "col")),
        check_vma=False,
    )
```

```python
import jax
import jax.numpy as jnp
from jax import lax
from jax.experimental import pallas as pl
from jax.experimental.pallas import tpu as pltpu
from jax.sharding import PartitionSpec as P

MESH = pl.DeviceIdType.MESH
NZ = 8
NPLANE = 32
NG = 16
ROWS = 16
LANES = 768
PIECES = 2
L = LANES // PIECES
OCTAVES = 24.0
TOP = 32767.0
TINY = 1.2e-38
GRANT = 24 * 1024 * 1024
GRANT2 = 16 * 1024 * 1024
STEPS = 2

PLANE = sorted(
    [(dx, dy, dc) for dx in range(4) for dy in range(4) for dc in range(2) if (dx, dy, dc) != (0, 0, 0)],
    key=lambda off: -(min(off[0], 4 - off[0]) + min(off[1], 4 - off[1])),
)
ZS = (1, 7, 2, 6, 3, 5, 4)


def iota(shape, dim):
    return lax.broadcasted_iota(jnp.int32, shape, dim)


def onehot(cond):
    return jnp.where(cond, 1.0, 0.0).astype(jnp.bfloat16)


def mm(a, b):
    return jnp.dot(a, b, preferred_element_type=jnp.float32)


def mm_nt(a, b):
    return lax.dot_general(a, b, (((1,), (1,)), ((), ())), preferred_element_type=jnp.float32)


def small(ints):
    return ints.astype(jnp.float32).astype(jnp.bfloat16)


def body(
    grad, count, rg_in, cg_in, codes, info,
    gv, rg, cg, mine, metas, zmine, zmetas, took, base, pick, spread, blend, part, ring, full, chosen,
    load_sem, small_sem, own_sem, meta_s, meta_r, zmeta_s, zmeta_r, a_s, a_r, up_s, up_r, dn_s, dn_r, g_s, g_r, b_s, b_r,
):
    row, col = lax.axis_index("row"), lax.axis_index("col")
    z, xl = row // 2, row % 2
    xh, y, c = col // 8, (col // 2) % 4, col % 2
    x = 2 * xh + xl
    q = xl * 16 + col

    def plane_peer(off):
        px, py, pc = (x + off[0]) % 4, (y + off[1]) % 4, (c + off[2]) % 2
        pcol = ((px // 2) * 4 + py) * 2 + pc
        return (2 * z + px % 2, pcol), (px % 2) * 16 + pcol

    def z_peer(dz):
        return (2 * ((z + dz) % NZ) + xl, col)

    def spot(which):
        return pl.multiple_of((which // 2) * ROWS, ROWS), (which % 2) * LANES

    def piece_of(which, p):
        r0, l0 = spot(which)
        return pl.ds(r0, ROWS), pl.ds(pl.multiple_of(l0 + p * L, 128), L)

    peers = [plane_peer(off) for off in PLANE]

    barrier = pltpu.get_barrier_semaphore()
    for dev, _ in peers:
        pl.semaphore_signal(barrier, inc=1, device_id=dev, device_id_type=MESH)
    for dz in ZS:
        pl.semaphore_signal(barrier, inc=1, device_id=z_peer(dz), device_id_type=MESH)

    load = pltpu.make_async_copy(grad, gv, load_sem)
    load.start()
    tables = [
        pltpu.make_async_copy(src, dst, small_sem.at[k])
        for k, (src, dst) in enumerate(((rg_in, rg), (cg_in, cg)))
    ]
    for table in tables:
        table.start()
    owns = []
    for p in range(PIECES):
        rs, ls = piece_of(q, p)
        own = pltpu.make_async_copy(grad.at[rs, ls], took.at[p, pl.ds(pl.multiple_of(q * ROWS, ROWS), ROWS)], own_sem.at[p])
        own.start()
        owns.append(own)

    load.wait()
    for table in tables:
        table.wait()
    largest = jnp.max(jnp.abs(gv[...].astype(jnp.float32)))
    own_w = count[...].astype(jnp.float32)
    mine[...] = jnp.where(iota((1, 128), 1) < 64, own_w, largest)

    pl.semaphore_wait(barrier, len(PLANE) + len(ZS))

    waits = []
    meta_bytes = metas.at[pl.ds(0, len(PLANE))]
    for dev, _ in peers:
        pltpu.make_async_remote_copy(
            src_ref=mine, dst_ref=metas.at[q], send_sem=meta_s, recv_sem=meta_r, device_id=dev, device_id_type=MESH
        ).start()
    for p in range(PIECES):
        for dev, pq in peers:
            rs, ls = piece_of(pq, p)
            pltpu.make_async_remote_copy(
                src_ref=gv.at[rs, ls],
                dst_ref=took.at[p, pl.ds(pl.multiple_of(q * ROWS, ROWS), ROWS)],
                send_sem=a_s.at[p], recv_sem=a_r.at[p], device_id=dev, device_id_type=MESH,
            ).start()
    metas[q] = mine[...]

    rg0, rg1, cg0 = small(rg[0]), small(rg[1]), small(cg[0])
    eye = onehot(iota((NG, NG), 0) == iota((NG, NG), 1))
    by_i = onehot(iota((256, NG), 0) // 16 == iota((256, NG), 1))
    j_of = (iota((256, NG), 0) % 16).astype(jnp.float32)
    first = onehot(mm(by_i, rg0) == j_of)
    last = onehot(mm(by_i, rg1) == j_of)
    n_i = onehot(iota((NG, 256), 1) // 16 == iota((NG, 256), 0))
    n_j = onehot(iota((NG, 256), 1) % 16 == iota((NG, 256), 0))
    cols_t = mm_nt(eye, cg0).astype(jnp.bfloat16)
    rows_t = mm_nt(eye, rg1).astype(jnp.bfloat16)
    middle = onehot(mm(cols_t, n_j) == (iota((NG, 256), 1) // 16).astype(jnp.float32))
    third = onehot(mm(rows_t, n_i) == (iota((NG, 256), 1) % 16).astype(jnp.float32))
    m2 = mm(middle, first).astype(jnp.bfloat16)
    m3 = mm_nt(third, middle).astype(jnp.bfloat16)
    m = mm(m3, m2)
    mb = m.astype(jnp.bfloat16)

    in_plane = onehot(iota((NPLANE, 256), 1) == iota((NPLANE, 256), 0) + 32 * z)
    first_z = mm(in_plane, first).astype(jnp.bfloat16)
    last_z = mm(in_plane, last).astype(jnp.bfloat16)
    row_g = onehot(iota((256, NG), 0) % 16 == iota((256, NG), 1))
    col_q = onehot(iota((NPLANE, 512), 1) // 16 == iota((NPLANE, 512), 0))
    wide = mm(mm_nt(row_g, first_z).astype(jnp.bfloat16), col_q)
    base[...] = jnp.where(iota((256, 512), 0) // 16 == iota((256, 512), 1) % 16, wide, 0.0)
    row_q = onehot(iota((512, NPLANE), 0) // 16 == iota((512, NPLANE), 1))
    col_k = onehot(iota((NG, 256), 1) % 16 == iota((NG, 256), 0))
    tall = mm(mm(row_q, last_z).astype(jnp.bfloat16), col_k)
    pick[...] = jnp.where(iota((512, 256), 0) % 16 == iota((512, 256), 1) // 16, tall, 0.0).astype(jnp.bfloat16)

    r32 = onehot(iota((32, NG), 0) % 16 == iota((32, NG), 1))
    c96 = onehot(iota((NG, 96), 1) % 16 == iota((NG, 96), 0))
    mix = mm(mm(r32, mb).astype(jnp.bfloat16), c96)
    blend[...] = jnp.where(iota((32, 96), 0) // 16 == (iota((32, 96), 1) // 16) % 2, mix, 0.0).astype(jnp.bfloat16)

    pltpu.make_async_copy(meta_bytes, meta_bytes, meta_r).wait()
    held = metas[:, 0, :]
    lane = iota((NPLANE, 128), 1)
    plane_w = jnp.sum(jnp.where(lane == iota((NPLANE, 128), 0), held[:, 0:1], 0.0), axis=0, keepdims=True)
    plane_x = jnp.max(jnp.where(lane >= 64, held, 0.0))
    zmine[...] = jnp.where(iota((1, 128), 1) < NPLANE, plane_w, plane_x)
    for dz in ZS:
        pltpu.make_async_remote_copy(
            src_ref=zmine, dst_ref=zmetas.at[z], send_sem=zmeta_s, recv_sem=zmeta_r, device_id=z_peer(dz), device_id_type=MESH
        ).start()
    zmetas[z] = zmine[...]
    w512 = mm(plane_w[:, 0:NPLANE].astype(jnp.bfloat16), col_q)
    spread[...] = (base[...] * w512).astype(jnp.bfloat16)

    def z_copy(p, up, step, src):
        s_sem, r_sem = (up_s, up_r) if up else (dn_s, dn_r)
        return pltpu.make_async_remote_copy(
            src_ref=src, dst_ref=ring.at[p, 0 if up else 1, step], send_sem=s_sem.at[p, step], recv_sem=r_sem.at[p, step],
            device_id=z_peer(1 if up else 7), device_id_type=MESH,
        )

    def chunk(dz):
        return pl.ds(pl.multiple_of(((z + dz) % NZ) * 32, 32), 32)

    def hops(p, up):
        return 4 if up == (p % 2 == 0) else 3

    sent = []

    def open_piece(p):
        owns[p].wait()
        got = took.at[p, pl.ds(0, len(PLANE) * ROWS)]
        pltpu.make_async_copy(got, got, a_r.at[p]).wait()
        part[p] = mm(spread[...], took[p])
        for up in (True, False):
            far = hops(p, up)
            cp = z_copy(p, up, 0, part.at[p, chunk(far if up else -far)])
            cp.start()
            sent.append(cp)

    def ring_step(p, step):
        for up in (True, False):
            far = hops(p, up)
            if step >= far:
                continue
            z_copy(p, up, step - 1, part.at[p, chunk(0)]).wait_recv()
            away = far - step
            slot = ring.at[p, 0 if up else 1, step - 1]
            slot[...] = slot[...] + part[p, chunk(away if up else -away), :]
            cp = z_copy(p, up, step, slot)
            cp.start()
            sent.append(cp)

    ztot = {}

    def totals_now():
        got = zmetas.at[pl.ds(0, NZ - 1)]
        pltpu.make_async_copy(got, got, zmeta_r).wait()
        cw = zmetas[:, 0, :]
        by_z = onehot(iota((256, NZ), 0) // 32 == iota((256, NZ), 1))
        lanes = iota((256, 128), 1)
        all_x = jnp.maximum(jnp.max(jnp.where(iota((NZ, 128), 1) >= NPLANE, cw, 0.0)), TINY)
        counts = jnp.where(iota((NZ, 128), 1) < NPLANE, cw, 0.0).astype(jnp.bfloat16)
        spread_w = mm(by_z, counts)
        w_col = jnp.sum(jnp.where(lanes == iota((256, 128), 0) % 32, spread_w, 0.0), axis=1, keepdims=True)
        c1 = jnp.sum(first.astype(jnp.float32) * w_col, axis=0, keepdims=True)
        c3 = jnp.sum(m * c1, axis=1, keepdims=True)
        ztot["x"] = all_x
        ztot["c3"] = jnp.concatenate([c3, c3], axis=0)
        is_me = onehot(iota((NG, NPLANE), 1) == q)
        mine_k = mm(is_me, last_z)
        own_c3 = jnp.sum(jnp.where(iota((NG, NG), 0) == iota((NG, NG), 1), mine_k, 0.0) * c3)
        info[...] = jnp.where(iota((8, 128), 1) < 64, own_c3, all_x)

    def mix_piece(p):
        for up in (True, False):
            z_copy(p, up, hops(p, up) - 1, part.at[p, chunk(0)]).wait_recv()
        total = part[p, chunk(0), :] + ring[p, 0, hops(p, True) - 1] + ring[p, 1, hops(p, False) - 1]
        hi = total.astype(jnp.bfloat16)
        rest = total - hi.astype(jnp.float32)
        mid = rest.astype(jnp.bfloat16)
        low = (rest - mid.astype(jnp.float32)).astype(jnp.bfloat16)
        mixed = mm(blend[...], jnp.concatenate([hi, mid, low], axis=0))
        avg = mixed / ztot["c3"]
        size = jnp.abs(avg) * (1.0 / ztot["x"])
        level = TOP + jnp.log2(jnp.maximum(size, 1e-30)) * (TOP / OCTAVES)
        level = jnp.clip(jnp.round(level), 0.0, TOP)
        full[p, chunk(0), :] = jnp.where(avg < 0, -level, level).astype(jnp.int32).astype(jnp.int16)
        for dz in ZS:
            pltpu.make_async_remote_copy(
                src_ref=full.at[p, chunk(0)], dst_ref=full.at[p, chunk(0)], send_sem=g_s.at[p], recv_sem=g_r.at[p],
                device_id=z_peer(dz), device_id_type=MESH,
            ).start()

    def send_piece(p):
        got = full.at[p, pl.ds(0, (NZ - 1) * 32)]
        pltpu.make_async_copy(got, got, g_r.at[p]).wait()
        code = full[p].astype(jnp.int32)
        high = code >> 8
        lows = code & 255
        high_sel = mm(pick[...], small(high))
        low_sel = mm(pick[...], small(lows))
        chosen[p] = (high_sel * 256.0 + low_sel).astype(jnp.int32).astype(jnp.int16)
        rs, ls = piece_of(q, p)
        for dev, pq in peers:
            pltpu.make_async_remote_copy(
                src_ref=chosen.at[p, pl.ds(pl.multiple_of(pq * ROWS, ROWS), ROWS)], dst_ref=codes.at[rs, ls],
                send_sem=b_s.at[p], recv_sem=b_r.at[p], device_id=dev, device_id_type=MESH,
            ).start()
        codes[rs, ls] = chosen[p, pl.ds(pl.multiple_of(q * ROWS, ROWS), ROWS), :]

    for t in range(PIECES + 4):
        for p in range(PIECES):
            step = t - p
            if 1 <= step <= 3:
                ring_step(p, step)
            elif step == 4:
                if p == 0:
                    totals_now()
                mix_piece(p)
        if t < PIECES:
            open_piece(t)
    for p in range(PIECES):
        send_piece(p)

    for p in range(PIECES):
        got = chosen.at[p, pl.ds(0, len(PLANE) * ROWS)]
        pltpu.make_async_copy(got, got, b_r.at[p]).wait()
    pltpu.make_async_copy(meta_bytes, meta_bytes, meta_s).wait()
    zm = zmetas.at[pl.ds(0, NZ - 1)]
    pltpu.make_async_copy(zm, zm, zmeta_s).wait()
    for cp in sent:
        cp.wait_send()
    for p in range(PIECES):
        a = took.at[p, pl.ds(0, len(PLANE) * ROWS)]
        pltpu.make_async_copy(a, a, a_s.at[p]).wait()
        g = full.at[p, pl.ds(0, (NZ - 1) * 32)]
        pltpu.make_async_copy(g, g, g_s.at[p]).wait()
        b = chosen.at[p, pl.ds(0, len(PLANE) * ROWS)]
        pltpu.make_async_copy(b, b, b_s.at[p]).wait()


def decode(codes, info, averaged, total):
    number = codes[...].astype(jnp.float32)
    size = info[0, 127] * jnp.exp2((jnp.abs(number) - TOP) * (OCTAVES / TOP))
    averaged[...] = jnp.where(number == 0, 0.0, jnp.where(number < 0, -size, size))
    total[...] = info[0:1, 0:1].astype(jnp.int32)


def stay(array):
    return pltpu.with_memory_space_constraint(array, pltpu.HBM)


def local(gradients, token_counts, row_groups, col_groups):
    flat = gradients.reshape(ROWS * 16, 2 * LANES)
    dma = pltpu.SemaphoreType.DMA
    vmem = pl.BlockSpec(memory_space=pltpu.VMEM)
    hbm = pl.BlockSpec(memory_space=pltpu.HBM)
    codes, info = pl.pallas_call(
        body,
        out_shape=(
            jax.ShapeDtypeStruct((256, 2 * LANES), jnp.int16),
            jax.ShapeDtypeStruct((8, 128), jnp.float32),
        ),
        in_specs=[hbm, pl.BlockSpec(memory_space=pltpu.VMEM), hbm, hbm],
        out_specs=(vmem, vmem),
        scratch_shapes=[
            pltpu.VMEM((256, 2 * LANES), jnp.bfloat16),
            pltpu.VMEM((2, NG, NG), jnp.int32),
            pltpu.VMEM((1, NG, NG), jnp.int32),
            pltpu.VMEM((1, 128), jnp.float32),
            pltpu.VMEM((NPLANE, 1, 128), jnp.float32),
            pltpu.VMEM((1, 128), jnp.float32),
            pltpu.VMEM((NZ, 1, 128), jnp.float32),
            pltpu.VMEM((PIECES, 512, L), jnp.bfloat16),
            pltpu.VMEM((256, 512), jnp.float32),
            pltpu.VMEM((512, 256), jnp.bfloat16),
            pltpu.VMEM((256, 512), jnp.bfloat16),
            pltpu.VMEM((32, 96), jnp.bfloat16),
            pltpu.VMEM((PIECES, 256, L), jnp.float32),
            pltpu.VMEM((PIECES, 2, 4, 32, L), jnp.float32),
            pltpu.VMEM((PIECES, 256, L), jnp.int16),
            pltpu.VMEM((PIECES, 512, L), jnp.int16),
            dma, dma((2,)), dma((PIECES,)), dma, dma, dma, dma,
            dma((PIECES,)), dma((PIECES,)),
            dma((PIECES, 4)), dma((PIECES, 4)), dma((PIECES, 4)), dma((PIECES, 4)),
            dma((PIECES,)), dma((PIECES,)), dma((PIECES,)), dma((PIECES,)),
        ],
        compiler_params=pltpu.CompilerParams(collective_id=0, has_side_effects=True, vmem_limit_bytes=GRANT),
        name="group_average",
    )(stay(flat), token_counts, stay(row_groups), stay(col_groups))
    averaged, total = pl.pallas_call(
        decode,
        grid=(STEPS,),
        out_shape=(
            jax.ShapeDtypeStruct((256, 2 * LANES), jnp.float32),
            jax.ShapeDtypeStruct((1, 1), jnp.int32),
        ),
        in_specs=[
            pl.BlockSpec((256 // STEPS, 2 * LANES), lambda s: (s, 0)),
            pl.BlockSpec((8, 128), lambda s: (0, 0)),
        ],
        out_specs=(
            pl.BlockSpec((256 // STEPS, 2 * LANES), lambda s: (s, 0)),
            pl.BlockSpec((1, 1), lambda s: (0, 0)),
        ),
        compiler_params=pltpu.CompilerParams(vmem_limit_bytes=GRANT2),
        name="decode",
    )(codes, info)
    return averaged.reshape(gradients.shape), total.reshape(token_counts.shape)


def solution(mesh):
    placed = (P("row", "col", None, None, None), P("row", "col"), P(), P())
    return jax.shard_map(
        local,
        mesh=mesh,
        in_specs=placed,
        out_specs=(P("row", "col", None, None, None), P("row", "col")),
        check_vma=False,
    )
```

```python
import jax
import jax.numpy as jnp
from jax import lax
from jax.experimental import pallas as pl
from jax.experimental.pallas import tpu as pltpu
from jax.sharding import PartitionSpec as P

MESH = pl.DeviceIdType.MESH
NZ = 8
NPLANE = 32
NG = 16
ROWS = 16
LANES = 768
WIDTHS = (384, 384)
PIECES = len(WIDTHS)
STARTS = tuple(sum(WIDTHS[:p]) for p in range(PIECES))
OCTAVES = 24.0
TOP = 32767.0
TINY = 1.2e-38
GRANT = 24 * 1024 * 1024
GRANT2 = 16 * 1024 * 1024
STEPS = 2

ORDER = (("open", 0), ("open", 1), ("relay", 0), ("totals", 0), ("relay", 1), ("mix", 0), ("mix", 1), ("pass", 0), ("pass", 1), ("send", 0), ("send", 1))
PLANE = sorted(
    [(dx, dy, dc) for dx in range(4) for dy in range(4) for dc in range(2) if (dx, dy, dc) != (0, 0, 0)],
    key=lambda off: -(min(off[0], 4 - off[0]) + min(off[1], 4 - off[1])),
)
ZS = (1, 7, 2, 6, 3, 5, 4)


def iota(shape, dim):
    return lax.broadcasted_iota(jnp.int32, shape, dim)


def onehot(cond):
    return jnp.where(cond, 1.0, 0.0).astype(jnp.bfloat16)


def mm(a, b):
    return jnp.dot(a, b, preferred_element_type=jnp.float32)


def mm_nt(a, b):
    return lax.dot_general(a, b, (((1,), (1,)), ((), ())), preferred_element_type=jnp.float32)


def small(ints):
    return ints.astype(jnp.float32).astype(jnp.bfloat16)


def body(
    grad, count, rg_in, cg_in, codes, info,
    gv, rg, cg, mine, metas, zmine, zmetas, took, base, pick, spread, blend, part, tree, full, chosen,
    load_sem, small_sem, own_sem, meta_s, meta_r, zmeta_s, zmeta_r, a_s, a_r, t_s, t_r, g_s, g_r, b_s, b_r,
):
    row, col = lax.axis_index("row"), lax.axis_index("col")
    z, xl = row // 2, row % 2
    xh, y, c = col // 8, (col // 2) % 4, col % 2
    x = 2 * xh + xl
    q = xl * 16 + col

    def plane_peer(off):
        px, py, pc = (x + off[0]) % 4, (y + off[1]) % 4, (c + off[2]) % 2
        pcol = ((px // 2) * 4 + py) * 2 + pc
        return (2 * z + px % 2, pcol), (px % 2) * 16 + pcol

    def z_peer(dz):
        return (2 * ((z + dz) % NZ) + xl, col)

    def spot(which):
        return pl.multiple_of((which // 2) * ROWS, ROWS), (which % 2) * LANES

    def piece_of(which, p):
        r0, l0 = spot(which)
        return pl.ds(r0, ROWS), pl.ds(pl.multiple_of(l0 + STARTS[p], 128), WIDTHS[p])

    lanes_of = [pl.ds(STARTS[p], WIDTHS[p]) for p in range(PIECES)]

    def block(which):
        return pl.ds(pl.multiple_of(which * ROWS, ROWS), ROWS)

    peers = [plane_peer(off) for off in PLANE]

    barrier = pltpu.get_barrier_semaphore()
    for dev, _ in peers:
        pl.semaphore_signal(barrier, inc=1, device_id=dev, device_id_type=MESH)
    for dz in ZS:
        pl.semaphore_signal(barrier, inc=1, device_id=z_peer(dz), device_id_type=MESH)

    load = pltpu.make_async_copy(grad, gv, load_sem)
    load.start()
    tables = [
        pltpu.make_async_copy(src, dst, small_sem.at[k])
        for k, (src, dst) in enumerate(((rg_in, rg), (cg_in, cg)))
    ]
    for table in tables:
        table.start()
    owns = []
    for p in range(PIECES):
        rs, ls = piece_of(q, p)
        own = pltpu.make_async_copy(grad.at[rs, ls], took.at[block(q), lanes_of[p]], own_sem.at[p])
        own.start()
        owns.append(own)

    load.wait()
    for table in tables:
        table.wait()
    largest = jnp.max(jnp.abs(gv[...].astype(jnp.float32)))
    own_w = count[...].astype(jnp.float32)
    mine[...] = jnp.where(iota((1, 128), 1) < 64, own_w, largest)

    pl.semaphore_wait(barrier, len(PLANE) + len(ZS))

    waits = []
    meta_bytes = metas.at[pl.ds(0, len(PLANE))]
    for dev, _ in peers:
        pltpu.make_async_remote_copy(
            src_ref=mine, dst_ref=metas.at[q], send_sem=meta_s, recv_sem=meta_r, device_id=dev, device_id_type=MESH
        ).start()
    for p in range(PIECES):
        for dev, pq in peers:
            rs, ls = piece_of(pq, p)
            pltpu.make_async_remote_copy(
                src_ref=gv.at[rs, ls],
                dst_ref=took.at[block(q), lanes_of[p]],
                send_sem=a_s.at[p], recv_sem=a_r.at[p], device_id=dev, device_id_type=MESH,
            ).start()
    metas[q] = mine[...]

    rg0, rg1, cg0 = small(rg[0]), small(rg[1]), small(cg[0])
    eye = onehot(iota((NG, NG), 0) == iota((NG, NG), 1))
    by_i = onehot(iota((256, NG), 0) // 16 == iota((256, NG), 1))
    j_of = (iota((256, NG), 0) % 16).astype(jnp.float32)
    first = onehot(mm(by_i, rg0) == j_of)
    last = onehot(mm(by_i, rg1) == j_of)
    n_i = onehot(iota((NG, 256), 1) // 16 == iota((NG, 256), 0))
    n_j = onehot(iota((NG, 256), 1) % 16 == iota((NG, 256), 0))
    cols_t = mm_nt(eye, cg0).astype(jnp.bfloat16)
    rows_t = mm_nt(eye, rg1).astype(jnp.bfloat16)
    middle = onehot(mm(cols_t, n_j) == (iota((NG, 256), 1) // 16).astype(jnp.float32))
    third = onehot(mm(rows_t, n_i) == (iota((NG, 256), 1) % 16).astype(jnp.float32))
    m2 = mm(middle, first).astype(jnp.bfloat16)
    m3 = mm_nt(third, middle).astype(jnp.bfloat16)
    m = mm(m3, m2)
    mb = m.astype(jnp.bfloat16)

    in_plane = onehot(iota((NPLANE, 256), 1) == iota((NPLANE, 256), 0) + 32 * z)
    first_z = mm(in_plane, first).astype(jnp.bfloat16)
    last_z = mm(in_plane, last).astype(jnp.bfloat16)
    row_g = onehot(iota((256, NG), 0) % 16 == iota((256, NG), 1))
    col_q = onehot(iota((NPLANE, 512), 1) // 16 == iota((NPLANE, 512), 0))
    wide = mm(mm_nt(row_g, first_z).astype(jnp.bfloat16), col_q)
    base[...] = jnp.where(iota((256, 512), 0) // 16 == iota((256, 512), 1) % 16, wide, 0.0)
    row_q = onehot(iota((512, NPLANE), 0) // 16 == iota((512, NPLANE), 1))
    col_k = onehot(iota((NG, 256), 1) % 16 == iota((NG, 256), 0))
    tall = mm(mm(row_q, last_z).astype(jnp.bfloat16), col_k)
    pick[...] = jnp.where(iota((512, 256), 0) % 16 == iota((512, 256), 1) // 16, tall, 0.0).astype(jnp.bfloat16)

    r32 = onehot(iota((32, NG), 0) % 16 == iota((32, NG), 1))
    c96 = onehot(iota((NG, 96), 1) % 16 == iota((NG, 96), 0))
    mix = mm(mm(r32, mb).astype(jnp.bfloat16), c96)
    blend[...] = jnp.where(iota((32, 96), 0) // 16 == (iota((32, 96), 1) // 16) % 2, mix, 0.0).astype(jnp.bfloat16)

    pltpu.make_async_copy(meta_bytes, meta_bytes, meta_r).wait()
    held = metas[:, 0, :]
    lane = iota((NPLANE, 128), 1)
    plane_w = jnp.sum(jnp.where(lane == iota((NPLANE, 128), 0), held[:, 0:1], 0.0), axis=0, keepdims=True)
    plane_x = jnp.max(jnp.where(lane >= 64, held, 0.0))
    zmine[...] = jnp.where(iota((1, 128), 1) < NPLANE, plane_w, plane_x)
    for dz in ZS:
        pltpu.make_async_remote_copy(
            src_ref=zmine, dst_ref=zmetas.at[z], send_sem=zmeta_s, recv_sem=zmeta_r, device_id=z_peer(dz), device_id_type=MESH
        ).start()
    zmetas[z] = zmine[...]
    w512 = mm(plane_w[:, 0:NPLANE].astype(jnp.bfloat16), col_q)
    spread[...] = (base[...] * w512).astype(jnp.bfloat16)

    def chunk(dz):
        return pl.ds(pl.multiple_of(((z + dz) % NZ) * 32, 32), 32)

    def side(p, dz):
        return dz if p % 2 == 0 else -dz

    sent = []

    def tree_copy(p, src, dz, slot):
        return pltpu.make_async_remote_copy(
            src_ref=src, dst_ref=tree.at[slot, :, lanes_of[p]], send_sem=t_s.at[p, slot], recv_sem=t_r.at[p, slot],
            device_id=z_peer(side(p, dz) % NZ), device_id_type=MESH,
        )

    def tree_send(p, src, dz, slot):
        cp = tree_copy(p, src, dz, slot)
        cp.start()
        sent.append(cp)

    def tree_wait(p, *slots):
        for slot in slots:
            tree_copy(p, part.at[chunk(0), lanes_of[p]], 1, slot).wait_recv()

    def own_part(p, dz):
        return part.at[chunk(side(p, dz)), lanes_of[p]]

    def open_piece(p):
        owns[p].wait()
        got = took.at[pl.ds(0, len(PLANE) * ROWS), lanes_of[p]]
        pltpu.make_async_copy(got, got, a_r.at[p]).wait()
        part[:, lanes_of[p]] = mm(spread[...], took[:, lanes_of[p]])
        tree_send(p, own_part(p, -4), -2, 2)
        tree_send(p, own_part(p, 3), 1, 0)
        tree_send(p, own_part(p, -3), -1, 1)
        tree_send(p, own_part(p, 1), 1, 3)
        tree_send(p, own_part(p, -1), -1, 4)

    def relay_piece(p):
        tree_wait(p, 0)
        tree[0, :, lanes_of[p]] = tree[0, :, lanes_of[p]] + own_part(p, 2)[...]
        tree_send(p, tree.at[0, :, lanes_of[p]], 2, 5)
        tree_wait(p, 1, 2)
        tree[1, :, lanes_of[p]] = tree[1, :, lanes_of[p]] + tree[2, :, lanes_of[p]] + own_part(p, -2)[...]
        tree_send(p, tree.at[1, :, lanes_of[p]], -2, 6)

    ztot = {}

    def totals_now():
        got = zmetas.at[pl.ds(0, NZ - 1)]
        pltpu.make_async_copy(got, got, zmeta_r).wait()
        cw = zmetas[:, 0, :]
        by_z = onehot(iota((256, NZ), 0) // 32 == iota((256, NZ), 1))
        lanes = iota((256, 128), 1)
        all_x = jnp.maximum(jnp.max(jnp.where(iota((NZ, 128), 1) >= NPLANE, cw, 0.0)), TINY)
        counts = jnp.where(iota((NZ, 128), 1) < NPLANE, cw, 0.0).astype(jnp.bfloat16)
        spread_w = mm(by_z, counts)
        w_col = jnp.sum(jnp.where(lanes == iota((256, 128), 0) % 32, spread_w, 0.0), axis=1, keepdims=True)
        c1 = jnp.sum(first.astype(jnp.float32) * w_col, axis=0, keepdims=True)
        c3 = jnp.sum(m * c1, axis=1, keepdims=True)
        ztot["x"] = all_x
        ztot["c3"] = jnp.concatenate([c3, c3], axis=0)
        is_me = onehot(iota((NG, NPLANE), 1) == q)
        mine_k = mm(is_me, last_z)
        own_c3 = jnp.sum(jnp.where(iota((NG, NG), 0) == iota((NG, NG), 1), mine_k, 0.0) * c3)
        info[...] = jnp.where(iota((8, 128), 1) < 64, own_c3, all_x)

    def full_copy(p, owner, dz, role):
        return pltpu.make_async_remote_copy(
            src_ref=full.at[chunk(owner), lanes_of[p]], dst_ref=full.at[chunk(owner), lanes_of[p]],
            send_sem=g_s.at[p, role], recv_sem=g_r.at[p, role], device_id=z_peer(side(p, dz) % NZ), device_id_type=MESH,
        )

    def full_send(p, owner, dz, role):
        cp = full_copy(p, side(p, owner), dz, role)
        cp.start()
        sent.append(cp)

    def full_wait(p, *roles):
        for role in roles:
            full_copy(p, 0, 1, role).wait_recv()

    def mix_piece(p):
        tree_wait(p, 3, 4, 5, 6)
        total = own_part(p, 0)[...]
        for slot in (3, 4, 5, 6):
            total = total + tree[slot, :, lanes_of[p]]
        hi = total.astype(jnp.bfloat16)
        rest = total - hi.astype(jnp.float32)
        mid = rest.astype(jnp.bfloat16)
        low = (rest - mid.astype(jnp.float32)).astype(jnp.bfloat16)
        mixed = mm(blend[...], jnp.concatenate([hi, mid, low], axis=0))
        avg = mixed / ztot["c3"]
        size = jnp.abs(avg) * (1.0 / ztot["x"])
        level = TOP + jnp.log2(jnp.maximum(size, 1e-30)) * (TOP / OCTAVES)
        level = jnp.clip(jnp.round(level), 0.0, TOP)
        full[chunk(0), lanes_of[p]] = jnp.where(avg < 0, -level, level).astype(jnp.int32).astype(jnp.int16)
        full_send(p, 0, 2, 2)
        full_send(p, 0, -2, 3)
        full_send(p, 0, 1, 0)
        full_send(p, 0, -1, 1)

    def pass_piece(p):
        full_wait(p, 2)
        full_send(p, -2, 2, 5)
        full_send(p, -2, 1, 4)
        full_wait(p, 3)
        full_send(p, 2, -1, 6)

    def send_piece(p):
        full_wait(p, 0, 1, 4, 5, 6)
        code = full[:, lanes_of[p]].astype(jnp.int32)
        high = code >> 8
        lows = code & 255
        high_sel = mm(pick[...], small(high))
        low_sel = mm(pick[...], small(lows))
        chosen[:, lanes_of[p]] = (high_sel * 256.0 + low_sel).astype(jnp.int32).astype(jnp.int16)
        rs, ls = piece_of(q, p)
        for dev, pq in peers:
            pltpu.make_async_remote_copy(
                src_ref=chosen.at[block(pq), lanes_of[p]], dst_ref=codes.at[rs, ls],
                send_sem=b_s.at[p], recv_sem=b_r.at[p], device_id=dev, device_id_type=MESH,
            ).start()
        codes[rs, ls] = chosen[block(q), lanes_of[p]]

    stages = {
        "open": open_piece, "relay": relay_piece, "mix": mix_piece, "pass": pass_piece, "send": send_piece,
        "totals": lambda p: totals_now(),
    }
    for name, p in ORDER:
        stages[name](p)

    rows31 = pl.ds(0, len(PLANE) * ROWS)
    for p in range(PIECES):
        got = chosen.at[rows31, lanes_of[p]]
        pltpu.make_async_copy(got, got, b_r.at[p]).wait()
    pltpu.make_async_copy(meta_bytes, meta_bytes, meta_s).wait()
    zm = zmetas.at[pl.ds(0, NZ - 1)]
    pltpu.make_async_copy(zm, zm, zmeta_s).wait()
    for cp in sent:
        cp.wait_send()
    for p in range(PIECES):
        a = took.at[rows31, lanes_of[p]]
        pltpu.make_async_copy(a, a, a_s.at[p]).wait()
        b = chosen.at[rows31, lanes_of[p]]
        pltpu.make_async_copy(b, b, b_s.at[p]).wait()


def decode(codes, info, averaged, total):
    number = codes[...].astype(jnp.float32)
    size = info[0, 127] * jnp.exp2((jnp.abs(number) - TOP) * (OCTAVES / TOP))
    averaged[...] = jnp.where(number == 0, 0.0, jnp.where(number < 0, -size, size))
    total[...] = info[0:1, 0:1].astype(jnp.int32)


def stay(array):
    return pltpu.with_memory_space_constraint(array, pltpu.HBM)


def local(gradients, token_counts, row_groups, col_groups):
    flat = gradients.reshape(ROWS * 16, 2 * LANES)
    dma = pltpu.SemaphoreType.DMA
    vmem = pl.BlockSpec(memory_space=pltpu.VMEM)
    hbm = pl.BlockSpec(memory_space=pltpu.HBM)
    codes, info = pl.pallas_call(
        body,
        out_shape=(
            jax.ShapeDtypeStruct((256, 2 * LANES), jnp.int16),
            jax.ShapeDtypeStruct((8, 128), jnp.float32),
        ),
        in_specs=[hbm, pl.BlockSpec(memory_space=pltpu.VMEM), hbm, hbm],
        out_specs=(vmem, vmem),
        scratch_shapes=[
            pltpu.VMEM((256, 2 * LANES), jnp.bfloat16),
            pltpu.VMEM((2, NG, NG), jnp.int32),
            pltpu.VMEM((1, NG, NG), jnp.int32),
            pltpu.VMEM((1, 128), jnp.float32),
            pltpu.VMEM((NPLANE, 1, 128), jnp.float32),
            pltpu.VMEM((1, 128), jnp.float32),
            pltpu.VMEM((NZ, 1, 128), jnp.float32),
            pltpu.VMEM((512, LANES), jnp.bfloat16),
            pltpu.VMEM((256, 512), jnp.float32),
            pltpu.VMEM((512, 256), jnp.bfloat16),
            pltpu.VMEM((256, 512), jnp.bfloat16),
            pltpu.VMEM((32, 96), jnp.bfloat16),
            pltpu.VMEM((256, LANES), jnp.float32),
            pltpu.VMEM((7, 32, LANES), jnp.float32),
            pltpu.VMEM((256, LANES), jnp.int16),
            pltpu.VMEM((512, LANES), jnp.int16),
            dma, dma((2,)), dma((PIECES,)), dma, dma, dma, dma,
            dma((PIECES,)), dma((PIECES,)),
            dma((PIECES, 7)), dma((PIECES, 7)), dma((PIECES, 7)), dma((PIECES, 7)),
            dma((PIECES,)), dma((PIECES,)),
        ],
        compiler_params=pltpu.CompilerParams(collective_id=0, has_side_effects=True, vmem_limit_bytes=GRANT),
        name="group_average",
    )(stay(flat), token_counts, stay(row_groups), stay(col_groups))
    averaged, total = pl.pallas_call(
        decode,
        grid=(STEPS,),
        out_shape=(
            jax.ShapeDtypeStruct((256, 2 * LANES), jnp.float32),
            jax.ShapeDtypeStruct((1, 1), jnp.int32),
        ),
        in_specs=[
            pl.BlockSpec((256 // STEPS, 2 * LANES), lambda s: (s, 0)),
            pl.BlockSpec((8, 128), lambda s: (0, 0)),
        ],
        out_specs=(
            pl.BlockSpec((256 // STEPS, 2 * LANES), lambda s: (s, 0)),
            pl.BlockSpec((1, 1), lambda s: (0, 0)),
        ),
        compiler_params=pltpu.CompilerParams(vmem_limit_bytes=GRANT2),
        name="decode",
    )(codes, info)
    return averaged.reshape(gradients.shape), total.reshape(token_counts.shape)


def solution(mesh):
    placed = (P("row", "col", None, None, None), P("row", "col"), P(), P())
    return jax.shard_map(
        local,
        mesh=mesh,
        in_specs=placed,
        out_specs=(P("row", "col", None, None, None), P("row", "col")),
        check_vma=False,
    )
```

```python
import jax
import jax.numpy as jnp
from jax import lax
from jax.experimental import pallas as pl
from jax.experimental.pallas import tpu as pltpu
from jax.sharding import PartitionSpec as P

MESH = pl.DeviceIdType.MESH
NZ = 8
NPLANE = 32
NG = 16
ROWS = 16
WIDTHS = (256, 256)
LANES = sum(WIDTHS)
SPLIT = 2 * LANES
REST = 1536 - SPLIT
PIECES = len(WIDTHS)
STARTS = tuple(sum(WIDTHS[:p]) for p in range(PIECES))
OCTAVES = 24.0
TOP = 32767.0
TINY = 1.2e-38
GRANT = 24 * 1024 * 1024
GRANT2 = 16 * 1024 * 1024
STEPS = 2

ORDER = (("open", 0), ("open", 1), ("totals", 0), ("far_open", 0), ("relay", 0), ("relay", 1), ("mix", 0), ("mix", 1), ("far_mix", 0), ("pass", 0), ("pass", 1), ("send", 0), ("far_send", 0), ("send", 1))
PLANE = sorted(
    [(dx, dy, dc) for dx in range(4) for dy in range(4) for dc in range(2) if (dx, dy, dc) != (0, 0, 0)],
    key=lambda off: -(min(off[0], 4 - off[0]) + min(off[1], 4 - off[1])),
)
ZS = (1, 7, 2, 6, 3, 5, 4)
COLUMN = [(dz, dc) for dz in (4, 3, 5, 2, 6, 1, 7, 0) for dc in (0, 1) if (dz, dc) != (0, 0)]
FLAT = [off[:2] for off in PLANE if off[2] == 0]


def iota(shape, dim):
    return lax.broadcasted_iota(jnp.int32, shape, dim)


def onehot(cond):
    return jnp.where(cond, 1.0, 0.0).astype(jnp.bfloat16)


def mm(a, b):
    return jnp.dot(a, b, preferred_element_type=jnp.float32)


def mm_nt(a, b):
    return lax.dot_general(a, b, (((1,), (1,)), ((), ())), preferred_element_type=jnp.float32)


def small(ints):
    return ints.astype(jnp.float32).astype(jnp.bfloat16)


def body(
    grad, count, rg_in, cg_in, codes, info,
    gv, rg, cg, mine, metas, zmine, zmetas, took, base, pick, spread, blend, part, tree, full, chosen,
    took2, base2, pick2, spread2, blend2, part2, gathered2, full2, chosen2,
    load_sem, small_sem, own_sem, meta_s, meta_r, zmeta_s, zmeta_r, a_s, a_r, t_s, t_r, g_s, g_r, b_s, b_r,
    own2_sem, a2_s, a2_r, t2_s, t2_r, g2_s, g2_r, b2_s, b2_r,
):
    row, col = lax.axis_index("row"), lax.axis_index("col")
    z, xl = row // 2, row % 2
    xh, y, c = col // 8, (col // 2) % 4, col % 2
    x = 2 * xh + xl
    q = xl * 16 + col

    def plane_peer(off):
        px, py, pc = (x + off[0]) % 4, (y + off[1]) % 4, (c + off[2]) % 2
        pcol = ((px // 2) * 4 + py) * 2 + pc
        return (2 * z + px % 2, pcol), (px % 2) * 16 + pcol

    def z_peer(dz):
        return (2 * ((z + dz) % NZ) + xl, col)

    def spot(which):
        return pl.multiple_of((which // 2) * ROWS, ROWS), (which % 2) * LANES

    def piece_of(which, p):
        r0, l0 = spot(which)
        return pl.ds(r0, ROWS), pl.ds(pl.multiple_of(l0 + STARTS[p], 128), WIDTHS[p])

    lanes_of = [pl.ds(STARTS[p], WIDTHS[p]) for p in range(PIECES)]

    def block(which):
        return pl.ds(pl.multiple_of(which * ROWS, ROWS), ROWS)

    def column_peer(off):
        pz, pc = (z + off[0]) % NZ, (c + off[1]) % 2
        return (2 * pz + xl, (xh * 4 + y) * 2 + pc), 2 * pz + pc

    def flat_peer(off):
        px, py = (x + off[0]) % 4, (y + off[1]) % 4
        return (2 * z + px % 2, ((px // 2) * 4 + py) * 2 + c), px * 4 + py

    e, m_at = 2 * z + c, 4 * x + y
    peers = [plane_peer(off) for off in PLANE]
    column = [column_peer(off) for off in COLUMN]
    flat = [flat_peer(off) for off in FLAT]
    others = [peer[0] for off, peer in zip(COLUMN, column) if off[0] and off[1]]
    rest = pl.ds(SPLIT, REST)

    load = pltpu.make_async_copy(grad, gv, load_sem)
    load.start()
    tables = [
        pltpu.make_async_copy(src, dst, small_sem.at[k])
        for k, (src, dst) in enumerate(((rg_in, rg), (cg_in, cg)))
    ]
    for table in tables:
        table.start()
    own2 = pltpu.make_async_copy(grad.at[block(e), rest], took2.at[block(e)], own2_sem)
    own2.start()
    owns = []
    for p in range(PIECES):
        rs, ls = piece_of(q, p)
        own = pltpu.make_async_copy(grad.at[rs, ls], took.at[block(q), lanes_of[p]], own_sem.at[p])
        own.start()
        owns.append(own)

    barrier = pltpu.get_barrier_semaphore()
    for dev, _ in peers:
        pl.semaphore_signal(barrier, inc=1, device_id=dev, device_id_type=MESH)
    for dz in ZS:
        pl.semaphore_signal(barrier, inc=1, device_id=z_peer(dz), device_id_type=MESH)
    for dev in others:
        pl.semaphore_signal(barrier, inc=1, device_id=dev, device_id_type=MESH)

    load.wait()
    for table in tables:
        table.wait()
    largest = jnp.max(jnp.abs(gv[...].astype(jnp.float32)))
    own_w = count[...].astype(jnp.float32)
    mine[...] = jnp.where(iota((1, 128), 1) < 64, own_w, largest)

    pl.semaphore_wait(barrier, len(PLANE) + len(ZS) + len(others))

    waits = []
    meta_bytes = metas.at[pl.ds(0, len(PLANE))]
    for dev, _ in peers:
        pltpu.make_async_remote_copy(
            src_ref=mine, dst_ref=metas.at[q], send_sem=meta_s, recv_sem=meta_r, device_id=dev, device_id_type=MESH
        ).start()
    for dev, pe in column:
        pltpu.make_async_remote_copy(
            src_ref=gv.at[block(pe), rest], dst_ref=took2.at[block(e)], send_sem=a2_s, recv_sem=a2_r,
            device_id=dev, device_id_type=MESH,
        ).start()
    for p in range(PIECES):
        for dev, pq in peers:
            rs, ls = piece_of(pq, p)
            pltpu.make_async_remote_copy(
                src_ref=gv.at[rs, ls],
                dst_ref=took.at[block(q), lanes_of[p]],
                send_sem=a_s.at[p], recv_sem=a_r.at[p], device_id=dev, device_id_type=MESH,
            ).start()
    metas[q] = mine[...]

    rg0, rg1, cg0 = small(rg[0]), small(rg[1]), small(cg[0])
    eye = onehot(iota((NG, NG), 0) == iota((NG, NG), 1))
    by_i = onehot(iota((256, NG), 0) // 16 == iota((256, NG), 1))
    j_of = (iota((256, NG), 0) % 16).astype(jnp.float32)
    first = onehot(mm(by_i, rg0) == j_of)
    last = onehot(mm(by_i, rg1) == j_of)
    n_i = onehot(iota((NG, 256), 1) // 16 == iota((NG, 256), 0))
    n_j = onehot(iota((NG, 256), 1) % 16 == iota((NG, 256), 0))
    cols_t = mm_nt(eye, cg0).astype(jnp.bfloat16)
    rows_t = mm_nt(eye, rg1).astype(jnp.bfloat16)
    middle = onehot(mm(cols_t, n_j) == (iota((NG, 256), 1) // 16).astype(jnp.float32))
    third = onehot(mm(rows_t, n_i) == (iota((NG, 256), 1) % 16).astype(jnp.float32))
    m2 = mm(middle, first).astype(jnp.bfloat16)
    m3 = mm_nt(third, middle).astype(jnp.bfloat16)
    m = mm(m3, m2)
    mb = m.astype(jnp.bfloat16)

    in_plane = onehot(iota((NPLANE, 256), 1) == iota((NPLANE, 256), 0) + 32 * z)
    first_z = mm(in_plane, first).astype(jnp.bfloat16)
    last_z = mm(in_plane, last).astype(jnp.bfloat16)
    row_g = onehot(iota((256, NG), 0) % 16 == iota((256, NG), 1))
    col_q = onehot(iota((NPLANE, 512), 1) // 16 == iota((NPLANE, 512), 0))
    wide = mm(mm_nt(row_g, first_z).astype(jnp.bfloat16), col_q)
    base[...] = jnp.where(iota((256, 512), 0) // 16 == iota((256, 512), 1) % 16, wide, 0.0)
    row_q = onehot(iota((512, NPLANE), 0) // 16 == iota((512, NPLANE), 1))
    col_k = onehot(iota((NG, 256), 1) % 16 == iota((NG, 256), 0))
    tall = mm(mm(row_q, last_z).astype(jnp.bfloat16), col_k)
    pick[...] = jnp.where(iota((512, 256), 0) % 16 == iota((512, 256), 1) // 16, tall, 0.0).astype(jnp.bfloat16)

    r32 = onehot(iota((32, NG), 0) % 16 == iota((32, NG), 1))
    c96 = onehot(iota((NG, 96), 1) % 16 == iota((NG, 96), 0))
    mix = mm(mm(r32, mb).astype(jnp.bfloat16), c96)
    blend[...] = jnp.where(iota((32, 96), 0) // 16 == (iota((32, 96), 1) // 16) % 2, mix, 0.0).astype(jnp.bfloat16)

    n_e = 32 * (iota((NG, 256), 0) // 2) + xl * 16 + (xh * 4 + y) * 2 + iota((NG, 256), 0) % 2
    in_column = onehot(iota((NG, 256), 1) == n_e)
    first_e = mm(in_column, first).astype(jnp.bfloat16)
    last_e = mm(in_column, last).astype(jnp.bfloat16)
    wide2 = mm(mm_nt(row_g, first_e).astype(jnp.bfloat16), n_i)
    base2[...] = jnp.where(iota((256, 256), 0) // 16 == iota((256, 256), 1) % 16, wide2, 0.0)
    tall2 = mm(mm(by_i, last_e).astype(jnp.bfloat16), col_k)
    pick2[...] = jnp.where(iota((256, 256), 0) % 16 == iota((256, 256), 1) // 16, tall2, 0.0).astype(jnp.bfloat16)
    blend2[...] = mm(mb, onehot(iota((NG, 48), 1) % 16 == iota((NG, 48), 0))).astype(jnp.bfloat16)

    pltpu.make_async_copy(meta_bytes, meta_bytes, meta_r).wait()
    held = metas[:, 0, :]
    lane = iota((NPLANE, 128), 1)
    plane_w = jnp.sum(jnp.where(lane == iota((NPLANE, 128), 0), held[:, 0:1], 0.0), axis=0, keepdims=True)
    plane_x = jnp.max(jnp.where(lane >= 64, held, 0.0))
    zmine[...] = jnp.where(iota((1, 128), 1) < NPLANE, plane_w, plane_x)
    for dz in ZS:
        pltpu.make_async_remote_copy(
            src_ref=zmine, dst_ref=zmetas.at[z], send_sem=zmeta_s, recv_sem=zmeta_r, device_id=z_peer(dz), device_id_type=MESH
        ).start()
    zmetas[z] = zmine[...]
    w512 = mm(plane_w[:, 0:NPLANE].astype(jnp.bfloat16), col_q)
    spread[...] = (base[...] * w512).astype(jnp.bfloat16)

    def chunk(dz):
        return pl.ds(pl.multiple_of(((z + dz) % NZ) * 32, 32), 32)

    def side(p, dz):
        return dz if p % 2 == 0 else -dz

    sent = []

    def tree_copy(p, src, dz, slot):
        return pltpu.make_async_remote_copy(
            src_ref=src, dst_ref=tree.at[slot, :, lanes_of[p]], send_sem=t_s.at[p, slot], recv_sem=t_r.at[p, slot],
            device_id=z_peer(side(p, dz) % NZ), device_id_type=MESH,
        )

    def tree_send(p, src, dz, slot):
        cp = tree_copy(p, src, dz, slot)
        cp.start()
        sent.append(cp)

    def tree_wait(p, *slots):
        for slot in slots:
            tree_copy(p, part.at[chunk(0), lanes_of[p]], 1, slot).wait_recv()

    def own_part(p, dz):
        return part.at[chunk(side(p, dz)), lanes_of[p]]

    def open_piece(p):
        owns[p].wait()
        got = took.at[pl.ds(0, len(PLANE) * ROWS), lanes_of[p]]
        pltpu.make_async_copy(got, got, a_r.at[p]).wait()
        part[:, lanes_of[p]] = mm(spread[...], took[:, lanes_of[p]])
        tree_send(p, own_part(p, -4), -2, 2)
        tree_send(p, own_part(p, 3), 1, 0)
        tree_send(p, own_part(p, -3), -1, 1)
        tree_send(p, own_part(p, 1), 1, 3)
        tree_send(p, own_part(p, -1), -1, 4)

    def relay_piece(p):
        tree_wait(p, 0)
        tree[0, :, lanes_of[p]] = tree[0, :, lanes_of[p]] + own_part(p, 2)[...]
        tree_send(p, tree.at[0, :, lanes_of[p]], 2, 5)
        tree_wait(p, 1, 2)
        tree[1, :, lanes_of[p]] = tree[1, :, lanes_of[p]] + tree[2, :, lanes_of[p]] + own_part(p, -2)[...]
        tree_send(p, tree.at[1, :, lanes_of[p]], -2, 6)

    ztot = {}

    def totals_now():
        got = zmetas.at[pl.ds(0, NZ - 1)]
        pltpu.make_async_copy(got, got, zmeta_r).wait()
        cw = zmetas[:, 0, :]
        by_z = onehot(iota((256, NZ), 0) // 32 == iota((256, NZ), 1))
        lanes = iota((256, 128), 1)
        all_x = jnp.maximum(jnp.max(jnp.where(iota((NZ, 128), 1) >= NPLANE, cw, 0.0)), TINY)
        counts = jnp.where(iota((NZ, 128), 1) < NPLANE, cw, 0.0).astype(jnp.bfloat16)
        spread_w = mm(by_z, counts)
        w_col = jnp.sum(jnp.where(lanes == iota((256, 128), 0) % 32, spread_w, 0.0), axis=1, keepdims=True)
        c1 = jnp.sum(first.astype(jnp.float32) * w_col, axis=0, keepdims=True)
        c3 = jnp.sum(m * c1, axis=1, keepdims=True)
        ztot["x"] = all_x
        ztot["c3_16"] = c3
        from_lane = onehot(iota((128, 256), 0) == xl * 16 + (xh * 4 + y) * 2 + (iota((128, 256), 1) // 16) % 2)
        w256 = jnp.where(iota((NZ, 256), 1) // 32 == iota((NZ, 256), 0), mm(counts, from_lane), 0.0)
        spread2[...] = (base2[...] * jnp.sum(w256, axis=0, keepdims=True)).astype(jnp.bfloat16)
        ztot["c3"] = jnp.concatenate([c3, c3], axis=0)
        is_me = onehot(iota((NG, NPLANE), 1) == q)
        mine_k = mm(is_me, last_z)
        own_c3 = jnp.sum(jnp.where(iota((NG, NG), 0) == iota((NG, NG), 1), mine_k, 0.0) * c3)
        info[...] = jnp.where(iota((8, 128), 1) < 64, own_c3, all_x)

    def coded(mixing, total, weights):
        hi = total.astype(jnp.bfloat16)
        after = total - hi.astype(jnp.float32)
        mid = after.astype(jnp.bfloat16)
        low = (after - mid.astype(jnp.float32)).astype(jnp.bfloat16)
        avg = mm(mixing[...], jnp.concatenate([hi, mid, low], axis=0)) / weights
        size = jnp.abs(avg) * (1.0 / ztot["x"])
        level = TOP + jnp.log2(jnp.maximum(size, 1e-30)) * (TOP / OCTAVES)
        level = jnp.clip(jnp.round(level), 0.0, TOP)
        return jnp.where(avg < 0, -level, level).astype(jnp.int32).astype(jnp.int16)

    def selected(picking, values):
        code = values.astype(jnp.int32)
        high = mm(picking[...], small(code >> 8))
        lows = mm(picking[...], small(code & 255))
        return (high * 256.0 + lows).astype(jnp.int32).astype(jnp.int16)

    def far_open(p):
        own2.wait()
        got = took2.at[pl.ds(0, len(COLUMN) * ROWS)]
        pltpu.make_async_copy(got, got, a2_r).wait()
        part2[...] = mm(spread2[...], took2[...])
        for dev, pm in flat:
            pltpu.make_async_remote_copy(
                src_ref=part2.at[block(pm)], dst_ref=gathered2.at[m_at], send_sem=t2_s, recv_sem=t2_r,
                device_id=dev, device_id_type=MESH,
            ).start()
        gathered2[m_at] = part2[block(m_at), :]

    def far_mix(p):
        got = gathered2.at[pl.ds(0, len(FLAT))]
        pltpu.make_async_copy(got, got, t2_r).wait()
        full2[block(m_at), :] = coded(blend2, jnp.sum(gathered2[...], axis=0), ztot["c3_16"])
        for dev, _ in flat:
            pltpu.make_async_remote_copy(
                src_ref=full2.at[block(m_at)], dst_ref=full2.at[block(m_at)], send_sem=g2_s, recv_sem=g2_r,
                device_id=dev, device_id_type=MESH,
            ).start()

    def far_send(p):
        got = full2.at[pl.ds(0, len(FLAT) * ROWS)]
        pltpu.make_async_copy(got, got, g2_r).wait()
        chosen2[...] = selected(pick2, full2[...])
        for dev, pe in column:
            pltpu.make_async_remote_copy(
                src_ref=chosen2.at[block(pe)], dst_ref=codes.at[block(e), rest], send_sem=b2_s, recv_sem=b2_r,
                device_id=dev, device_id_type=MESH,
            ).start()
        codes[block(e), rest] = chosen2[block(e), :]

    def full_copy(p, owner, dz, role):
        return pltpu.make_async_remote_copy(
            src_ref=full.at[chunk(owner), lanes_of[p]], dst_ref=full.at[chunk(owner), lanes_of[p]],
            send_sem=g_s.at[p, role], recv_sem=g_r.at[p, role], device_id=z_peer(side(p, dz) % NZ), device_id_type=MESH,
        )

    def full_send(p, owner, dz, role):
        cp = full_copy(p, side(p, owner), dz, role)
        cp.start()
        sent.append(cp)

    def full_wait(p, *roles):
        for role in roles:
            full_copy(p, 0, 1, role).wait_recv()

    def mix_piece(p):
        tree_wait(p, 3, 4, 5, 6)
        total = own_part(p, 0)[...]
        for slot in (3, 4, 5, 6):
            total = total + tree[slot, :, lanes_of[p]]
        full[chunk(0), lanes_of[p]] = coded(blend, total, ztot["c3"])
        full_send(p, 0, 2, 2)
        full_send(p, 0, -2, 3)
        full_send(p, 0, 1, 0)
        full_send(p, 0, -1, 1)

    def pass_piece(p):
        full_wait(p, 2)
        full_send(p, -2, 2, 5)
        full_send(p, -2, 1, 4)
        full_wait(p, 3)
        full_send(p, 2, -1, 6)

    def send_piece(p):
        full_wait(p, 0, 1, 4, 5, 6)
        chosen[:, lanes_of[p]] = selected(pick, full[:, lanes_of[p]])
        rs, ls = piece_of(q, p)
        for dev, pq in peers:
            pltpu.make_async_remote_copy(
                src_ref=chosen.at[block(pq), lanes_of[p]], dst_ref=codes.at[rs, ls],
                send_sem=b_s.at[p], recv_sem=b_r.at[p], device_id=dev, device_id_type=MESH,
            ).start()
        codes[rs, ls] = chosen[block(q), lanes_of[p]]

    stages = {
        "open": open_piece, "relay": relay_piece, "mix": mix_piece, "pass": pass_piece, "send": send_piece,
        "totals": lambda p: totals_now(), "far_open": far_open, "far_mix": far_mix, "far_send": far_send,
    }
    for name, p in ORDER:
        stages[name](p)

    rows31 = pl.ds(0, len(PLANE) * ROWS)
    for p in range(PIECES):
        got = chosen.at[rows31, lanes_of[p]]
        pltpu.make_async_copy(got, got, b_r.at[p]).wait()
    got2 = chosen2.at[pl.ds(0, len(COLUMN) * ROWS)]
    pltpu.make_async_copy(got2, got2, b2_r).wait()
    pltpu.make_async_copy(got2, got2, b2_s).wait()
    a2 = took2.at[pl.ds(0, len(COLUMN) * ROWS)]
    pltpu.make_async_copy(a2, a2, a2_s).wait()
    t2 = gathered2.at[pl.ds(0, len(FLAT))]
    pltpu.make_async_copy(t2, t2, t2_s).wait()
    g2 = full2.at[pl.ds(0, len(FLAT) * ROWS)]
    pltpu.make_async_copy(g2, g2, g2_s).wait()
    pltpu.make_async_copy(meta_bytes, meta_bytes, meta_s).wait()
    zm = zmetas.at[pl.ds(0, NZ - 1)]
    pltpu.make_async_copy(zm, zm, zmeta_s).wait()
    for cp in sent:
        cp.wait_send()
    for p in range(PIECES):
        a = took.at[rows31, lanes_of[p]]
        pltpu.make_async_copy(a, a, a_s.at[p]).wait()
        b = chosen.at[rows31, lanes_of[p]]
        pltpu.make_async_copy(b, b, b_s.at[p]).wait()


def decode(codes, info, averaged, total):
    number = codes[...].astype(jnp.float32)
    size = info[0, 127] * jnp.exp2((jnp.abs(number) - TOP) * (OCTAVES / TOP))
    averaged[...] = jnp.where(number == 0, 0.0, jnp.where(number < 0, -size, size))
    total[...] = info[0:1, 0:1].astype(jnp.int32)


def stay(array):
    return pltpu.with_memory_space_constraint(array, pltpu.HBM)


def local(gradients, token_counts, row_groups, col_groups):
    flat = gradients.reshape(256, 1536)
    dma = pltpu.SemaphoreType.DMA
    vmem = pl.BlockSpec(memory_space=pltpu.VMEM)
    hbm = pl.BlockSpec(memory_space=pltpu.HBM)
    codes, info = pl.pallas_call(
        body,
        out_shape=(
            jax.ShapeDtypeStruct((256, 1536), jnp.int16),
            jax.ShapeDtypeStruct((8, 128), jnp.float32),
        ),
        in_specs=[hbm, pl.BlockSpec(memory_space=pltpu.VMEM), hbm, hbm],
        out_specs=(vmem, vmem),
        scratch_shapes=[
            pltpu.VMEM((256, 1536), jnp.bfloat16),
            pltpu.VMEM((2, NG, NG), jnp.int32),
            pltpu.VMEM((1, NG, NG), jnp.int32),
            pltpu.VMEM((1, 128), jnp.float32),
            pltpu.VMEM((NPLANE, 1, 128), jnp.float32),
            pltpu.VMEM((1, 128), jnp.float32),
            pltpu.VMEM((NZ, 1, 128), jnp.float32),
            pltpu.VMEM((512, LANES), jnp.bfloat16),
            pltpu.VMEM((256, 512), jnp.float32),
            pltpu.VMEM((512, 256), jnp.bfloat16),
            pltpu.VMEM((256, 512), jnp.bfloat16),
            pltpu.VMEM((32, 96), jnp.bfloat16),
            pltpu.VMEM((256, LANES), jnp.float32),
            pltpu.VMEM((7, 32, LANES), jnp.float32),
            pltpu.VMEM((256, LANES), jnp.int16),
            pltpu.VMEM((512, LANES), jnp.int16),
            pltpu.VMEM((256, REST), jnp.bfloat16),
            pltpu.VMEM((256, 256), jnp.float32),
            pltpu.VMEM((256, 256), jnp.bfloat16),
            pltpu.VMEM((256, 256), jnp.bfloat16),
            pltpu.VMEM((NG, 48), jnp.bfloat16),
            pltpu.VMEM((256, REST), jnp.float32),
            pltpu.VMEM((NG, NG, REST), jnp.float32),
            pltpu.VMEM((256, REST), jnp.int16),
            pltpu.VMEM((256, REST), jnp.int16),
            dma, dma((2,)), dma((PIECES,)), dma, dma, dma, dma,
            dma((PIECES,)), dma((PIECES,)),
            dma((PIECES, 7)), dma((PIECES, 7)), dma((PIECES, 7)), dma((PIECES, 7)),
            dma((PIECES,)), dma((PIECES,)),
            dma, dma, dma, dma, dma, dma, dma, dma, dma,
        ],
        compiler_params=pltpu.CompilerParams(collective_id=0, has_side_effects=True, vmem_limit_bytes=GRANT),
        name="group_average",
    )(stay(flat), token_counts, stay(row_groups), stay(col_groups))
    averaged, total = pl.pallas_call(
        decode,
        grid=(STEPS,),
        out_shape=(
            jax.ShapeDtypeStruct((256, 1536), jnp.float32),
            jax.ShapeDtypeStruct((1, 1), jnp.int32),
        ),
        in_specs=[
            pl.BlockSpec((256 // STEPS, 1536), lambda s: (s, 0)),
            pl.BlockSpec((8, 128), lambda s: (0, 0)),
        ],
        out_specs=(
            pl.BlockSpec((256 // STEPS, 1536), lambda s: (s, 0)),
            pl.BlockSpec((1, 1), lambda s: (0, 0)),
        ),
        compiler_params=pltpu.CompilerParams(vmem_limit_bytes=GRANT2),
        name="decode",
    )(codes, info)
    return averaged.reshape(gradients.shape), total.reshape(token_counts.shape)


def solution(mesh):
    placed = (P("row", "col", None, None, None), P("row", "col"), P(), P())
    return jax.shard_map(
        local,
        mesh=mesh,
        in_specs=placed,
        out_specs=(P("row", "col", None, None, None), P("row", "col")),
        check_vma=False,
    )
```

```python
import jax
import jax.numpy as jnp
from jax import lax
from jax.experimental import pallas as pl
from jax.experimental.pallas import tpu as pltpu
from jax.sharding import PartitionSpec as P

MESH = pl.DeviceIdType.MESH
NZ = 8
NPLANE = 32
NG = 16
ROWS = 16
WIDTHS = (256, 256)
LANES = sum(WIDTHS)
SPLIT = 2 * LANES
REST = 1536 - SPLIT
FAR = 2
FARW = REST // FAR
PIECES = len(WIDTHS)
STARTS = tuple(sum(WIDTHS[:p]) for p in range(PIECES))
OCTAVES = 24.0
TOP = 32767.0
TINY = 1.2e-38
GRANT = 24 * 1024 * 1024
GRANT2 = 16 * 1024 * 1024
STEPS = 2

ORDER = (("open", 0), ("open", 1), ("far_weights", 0), ("far_open", 0), ("far_open", 1), ("relay", 0), ("relay", 1), ("totals", 0), ("mix", 0), ("mix", 1), ("far_mix", 0), ("far_mix", 1), ("pass", 0), ("pass", 1), ("send", 0), ("far_send", 0), ("far_send", 1), ("send", 1))
PLANE = sorted(
    [(dx, dy, dc) for dx in range(4) for dy in range(4) for dc in range(2) if (dx, dy, dc) != (0, 0, 0)],
    key=lambda off: -(min(off[0], 4 - off[0]) + min(off[1], 4 - off[1])),
)
ZS = (1, 7, 2, 6, 3, 5, 4)
COLUMN = [(dz, dc) for dz in (4, 3, 5, 2, 6, 1, 7, 0) for dc in (0, 1) if (dz, dc) != (0, 0)]
FLAT = [off[:2] for off in PLANE if off[2] == 0]


def iota(shape, dim):
    return lax.broadcasted_iota(jnp.int32, shape, dim)


def onehot(cond):
    return jnp.where(cond, 1.0, 0.0).astype(jnp.bfloat16)


def mm(a, b):
    return jnp.dot(a, b, preferred_element_type=jnp.float32)


def mm_nt(a, b):
    return lax.dot_general(a, b, (((1,), (1,)), ((), ())), preferred_element_type=jnp.float32)


def small(ints):
    return ints.astype(jnp.float32).astype(jnp.bfloat16)


def body(
    grad, count, rg_in, cg_in, codes, info,
    gv, rg, cg, mine, metas, zmine, zmetas, took, base, pick, spread, blend, part, tree, full, chosen,
    metas2, took2, base2, pick2, spread2, blend2, part2, gathered2, full2, chosen2,
    load_sem, small_sem, own_sem, meta_s, meta_r, zmeta_s, zmeta_r, a_s, a_r, t_s, t_r, g_s, g_r, b_s, b_r,
    own2_sem, a2_s, a2_r, t2_s, t2_r, g2_s, g2_r, b2_s, b2_r, meta2_s, meta2_r,
):
    row, col = lax.axis_index("row"), lax.axis_index("col")
    z, xl = row // 2, row % 2
    xh, y, c = col // 8, (col // 2) % 4, col % 2
    x = 2 * xh + xl
    q = xl * 16 + col

    def plane_peer(off):
        px, py, pc = (x + off[0]) % 4, (y + off[1]) % 4, (c + off[2]) % 2
        pcol = ((px // 2) * 4 + py) * 2 + pc
        return (2 * z + px % 2, pcol), (px % 2) * 16 + pcol

    def z_peer(dz):
        return (2 * ((z + dz) % NZ) + xl, col)

    def spot(which):
        return pl.multiple_of((which // 2) * ROWS, ROWS), (which % 2) * LANES

    def piece_of(which, p):
        r0, l0 = spot(which)
        return pl.ds(r0, ROWS), pl.ds(pl.multiple_of(l0 + STARTS[p], 128), WIDTHS[p])

    lanes_of = [pl.ds(STARTS[p], WIDTHS[p]) for p in range(PIECES)]

    def block(which):
        return pl.ds(pl.multiple_of(which * ROWS, ROWS), ROWS)

    def column_peer(off):
        pz, pc = (z + off[0]) % NZ, (c + off[1]) % 2
        return (2 * pz + xl, (xh * 4 + y) * 2 + pc), 2 * pz + pc

    def flat_peer(off):
        px, py = (x + off[0]) % 4, (y + off[1]) % 4
        return (2 * z + px % 2, ((px // 2) * 4 + py) * 2 + c), px * 4 + py

    e, m_at = 2 * z + c, 4 * x + y
    peers = [plane_peer(off) for off in PLANE]
    column = [column_peer(off) for off in COLUMN]
    flat = [flat_peer(off) for off in FLAT]
    others = [peer[0] for off, peer in zip(COLUMN, column) if off[0] and off[1]]
    rest = [pl.ds(SPLIT + p * FARW, FARW) for p in range(FAR)]
    far = [pl.ds(p * FARW, FARW) for p in range(FAR)]

    load = pltpu.make_async_copy(grad, gv, load_sem)
    load.start()
    tables = [
        pltpu.make_async_copy(src, dst, small_sem.at[k])
        for k, (src, dst) in enumerate(((rg_in, rg), (cg_in, cg)))
    ]
    for table in tables:
        table.start()
    own2 = []
    for p in range(FAR):
        own2.append(pltpu.make_async_copy(grad.at[block(e), rest[p]], took2.at[block(e), far[p]], own2_sem.at[p]))
        own2[p].start()
    owns = []
    for p in range(PIECES):
        rs, ls = piece_of(q, p)
        own = pltpu.make_async_copy(grad.at[rs, ls], took.at[block(q), lanes_of[p]], own_sem.at[p])
        own.start()
        owns.append(own)

    barrier = pltpu.get_barrier_semaphore()
    for dev, _ in peers:
        pl.semaphore_signal(barrier, inc=1, device_id=dev, device_id_type=MESH)
    for dz in ZS:
        pl.semaphore_signal(barrier, inc=1, device_id=z_peer(dz), device_id_type=MESH)
    for dev in others:
        pl.semaphore_signal(barrier, inc=1, device_id=dev, device_id_type=MESH)

    load.wait()
    for table in tables:
        table.wait()
    largest = jnp.max(jnp.abs(gv[...].astype(jnp.float32)))
    own_w = count[...].astype(jnp.float32)
    mine[...] = jnp.where(iota((1, 128), 1) < 64, own_w, largest)

    pl.semaphore_wait(barrier, len(PLANE) + len(ZS) + len(others))

    waits = []
    meta_bytes = metas.at[pl.ds(0, len(PLANE))]
    for dev, _ in peers:
        pltpu.make_async_remote_copy(
            src_ref=mine, dst_ref=metas.at[q], send_sem=meta_s, recv_sem=meta_r, device_id=dev, device_id_type=MESH
        ).start()
    for dev, _ in column:
        pltpu.make_async_remote_copy(
            src_ref=mine, dst_ref=metas2.at[e], send_sem=meta2_s, recv_sem=meta2_r, device_id=dev, device_id_type=MESH
        ).start()
    for p in range(max(PIECES, FAR)):
        if p < FAR:
            for dev, pe in column:
                pltpu.make_async_remote_copy(
                    src_ref=gv.at[block(pe), rest[p]], dst_ref=took2.at[block(e), far[p]], send_sem=a2_s.at[p],
                    recv_sem=a2_r.at[p], device_id=dev, device_id_type=MESH,
                ).start()
        if p < PIECES:
            for dev, pq in peers:
                rs, ls = piece_of(pq, p)
                pltpu.make_async_remote_copy(
                    src_ref=gv.at[rs, ls], dst_ref=took.at[block(q), lanes_of[p]],
                    send_sem=a_s.at[p], recv_sem=a_r.at[p], device_id=dev, device_id_type=MESH,
                ).start()
    metas[q] = mine[...]
    metas2[e] = mine[...]

    rg0, rg1, cg0 = small(rg[0]), small(rg[1]), small(cg[0])
    eye = onehot(iota((NG, NG), 0) == iota((NG, NG), 1))
    by_i = onehot(iota((256, NG), 0) // 16 == iota((256, NG), 1))
    j_of = (iota((256, NG), 0) % 16).astype(jnp.float32)
    first = onehot(mm(by_i, rg0) == j_of)
    last = onehot(mm(by_i, rg1) == j_of)
    n_i = onehot(iota((NG, 256), 1) // 16 == iota((NG, 256), 0))
    n_j = onehot(iota((NG, 256), 1) % 16 == iota((NG, 256), 0))
    cols_t = mm_nt(eye, cg0).astype(jnp.bfloat16)
    rows_t = mm_nt(eye, rg1).astype(jnp.bfloat16)
    middle = onehot(mm(cols_t, n_j) == (iota((NG, 256), 1) // 16).astype(jnp.float32))
    third = onehot(mm(rows_t, n_i) == (iota((NG, 256), 1) % 16).astype(jnp.float32))
    m2 = mm(middle, first).astype(jnp.bfloat16)
    m3 = mm_nt(third, middle).astype(jnp.bfloat16)
    m = mm(m3, m2)
    mb = m.astype(jnp.bfloat16)

    in_plane = onehot(iota((NPLANE, 256), 1) == iota((NPLANE, 256), 0) + 32 * z)
    first_z = mm(in_plane, first).astype(jnp.bfloat16)
    last_z = mm(in_plane, last).astype(jnp.bfloat16)
    row_g = onehot(iota((256, NG), 0) % 16 == iota((256, NG), 1))
    col_q = onehot(iota((NPLANE, 512), 1) // 16 == iota((NPLANE, 512), 0))
    wide = mm(mm_nt(row_g, first_z).astype(jnp.bfloat16), col_q)
    base[...] = jnp.where(iota((256, 512), 0) // 16 == iota((256, 512), 1) % 16, wide, 0.0)
    row_q = onehot(iota((512, NPLANE), 0) // 16 == iota((512, NPLANE), 1))
    col_k = onehot(iota((NG, 256), 1) % 16 == iota((NG, 256), 0))
    tall = mm(mm(row_q, last_z).astype(jnp.bfloat16), col_k)
    pick[...] = jnp.where(iota((512, 256), 0) % 16 == iota((512, 256), 1) // 16, tall, 0.0).astype(jnp.bfloat16)

    r32 = onehot(iota((32, NG), 0) % 16 == iota((32, NG), 1))
    c96 = onehot(iota((NG, 96), 1) % 16 == iota((NG, 96), 0))
    mix = mm(mm(r32, mb).astype(jnp.bfloat16), c96)
    blend[...] = jnp.where(iota((32, 96), 0) // 16 == (iota((32, 96), 1) // 16) % 2, mix, 0.0).astype(jnp.bfloat16)

    n_e = 32 * (iota((NG, 256), 0) // 2) + xl * 16 + (xh * 4 + y) * 2 + iota((NG, 256), 0) % 2
    in_column = onehot(iota((NG, 256), 1) == n_e)
    first_e = mm(in_column, first).astype(jnp.bfloat16)
    last_e = mm(in_column, last).astype(jnp.bfloat16)
    wide2 = mm(mm_nt(row_g, first_e).astype(jnp.bfloat16), n_i)
    base2[...] = jnp.where(iota((256, 256), 0) // 16 == iota((256, 256), 1) % 16, wide2, 0.0)
    tall2 = mm(mm(by_i, last_e).astype(jnp.bfloat16), col_k)
    pick2[...] = jnp.where(iota((256, 256), 0) % 16 == iota((256, 256), 1) // 16, tall2, 0.0).astype(jnp.bfloat16)
    blend2[...] = mm(mb, onehot(iota((NG, 48), 1) % 16 == iota((NG, 48), 0))).astype(jnp.bfloat16)

    pltpu.make_async_copy(meta_bytes, meta_bytes, meta_r).wait()
    held = metas[:, 0, :]
    lane = iota((NPLANE, 128), 1)
    plane_w = jnp.sum(jnp.where(lane == iota((NPLANE, 128), 0), held[:, 0:1], 0.0), axis=0, keepdims=True)
    plane_x = jnp.max(jnp.where(lane >= 64, held, 0.0))
    zmine[...] = jnp.where(iota((1, 128), 1) < NPLANE, plane_w, plane_x)
    for dz in ZS:
        pltpu.make_async_remote_copy(
            src_ref=zmine, dst_ref=zmetas.at[z], send_sem=zmeta_s, recv_sem=zmeta_r, device_id=z_peer(dz), device_id_type=MESH
        ).start()
    zmetas[z] = zmine[...]
    w512 = mm(plane_w[:, 0:NPLANE].astype(jnp.bfloat16), col_q)
    spread[...] = (base[...] * w512).astype(jnp.bfloat16)

    def chunk(dz):
        return pl.ds(pl.multiple_of(((z + dz) % NZ) * 32, 32), 32)

    def side(p, dz):
        return dz if p % 2 == 0 else -dz

    sent = []

    def tree_copy(p, src, dz, slot):
        return pltpu.make_async_remote_copy(
            src_ref=src, dst_ref=tree.at[slot, :, lanes_of[p]], send_sem=t_s.at[p, slot], recv_sem=t_r.at[p, slot],
            device_id=z_peer(side(p, dz) % NZ), device_id_type=MESH,
        )

    def tree_send(p, src, dz, slot):
        cp = tree_copy(p, src, dz, slot)
        cp.start()
        sent.append(cp)

    def tree_wait(p, *slots):
        for slot in slots:
            tree_copy(p, part.at[chunk(0), lanes_of[p]], 1, slot).wait_recv()

    def own_part(p, dz):
        return part.at[chunk(side(p, dz)), lanes_of[p]]

    def open_piece(p):
        owns[p].wait()
        got = took.at[pl.ds(0, len(PLANE) * ROWS), lanes_of[p]]
        pltpu.make_async_copy(got, got, a_r.at[p]).wait()
        part[:, lanes_of[p]] = mm(spread[...], took[:, lanes_of[p]])
        tree_send(p, own_part(p, -4), -2, 2)
        tree_send(p, own_part(p, 3), 1, 0)
        tree_send(p, own_part(p, -3), -1, 1)
        tree_send(p, own_part(p, 1), 1, 3)
        tree_send(p, own_part(p, -1), -1, 4)

    def relay_piece(p):
        tree_wait(p, 0)
        tree[0, :, lanes_of[p]] = tree[0, :, lanes_of[p]] + own_part(p, 2)[...]
        tree_send(p, tree.at[0, :, lanes_of[p]], 2, 5)
        tree_wait(p, 1, 2)
        tree[1, :, lanes_of[p]] = tree[1, :, lanes_of[p]] + tree[2, :, lanes_of[p]] + own_part(p, -2)[...]
        tree_send(p, tree.at[1, :, lanes_of[p]], -2, 6)

    ztot = {}

    def totals_now():
        got = zmetas.at[pl.ds(0, NZ - 1)]
        pltpu.make_async_copy(got, got, zmeta_r).wait()
        cw = zmetas[:, 0, :]
        by_z = onehot(iota((256, NZ), 0) // 32 == iota((256, NZ), 1))
        lanes = iota((256, 128), 1)
        all_x = jnp.maximum(jnp.max(jnp.where(iota((NZ, 128), 1) >= NPLANE, cw, 0.0)), TINY)
        counts = jnp.where(iota((NZ, 128), 1) < NPLANE, cw, 0.0).astype(jnp.bfloat16)
        spread_w = mm(by_z, counts)
        w_col = jnp.sum(jnp.where(lanes == iota((256, 128), 0) % 32, spread_w, 0.0), axis=1, keepdims=True)
        c1 = jnp.sum(first.astype(jnp.float32) * w_col, axis=0, keepdims=True)
        c3 = jnp.sum(m * c1, axis=1, keepdims=True)
        ztot["x"] = all_x
        ztot["c3_16"] = c3
        ztot["c3"] = jnp.concatenate([c3, c3], axis=0)
        is_me = onehot(iota((NG, NPLANE), 1) == q)
        mine_k = mm(is_me, last_z)
        own_c3 = jnp.sum(jnp.where(iota((NG, NG), 0) == iota((NG, NG), 1), mine_k, 0.0) * c3)
        info[...] = jnp.where(iota((8, 128), 1) < 64, own_c3, all_x)

    def coded(mixing, total, weights):
        hi = total.astype(jnp.bfloat16)
        after = total - hi.astype(jnp.float32)
        mid = after.astype(jnp.bfloat16)
        low = (after - mid.astype(jnp.float32)).astype(jnp.bfloat16)
        avg = mm(mixing[...], jnp.concatenate([hi, mid, low], axis=0)) / weights
        size = jnp.abs(avg) * (1.0 / ztot["x"])
        level = TOP + jnp.log2(jnp.maximum(size, 1e-30)) * (TOP / OCTAVES)
        level = jnp.clip(jnp.round(level), 0.0, TOP)
        return jnp.where(avg < 0, -level, level).astype(jnp.int32).astype(jnp.int16)

    def selected(picking, values):
        code = values.astype(jnp.int32)
        high = mm(picking[...], small(code >> 8))
        lows = mm(picking[...], small(code & 255))
        return (high * 256.0 + lows).astype(jnp.int32).astype(jnp.int16)

    def far_weights(p):
        got = metas2.at[pl.ds(0, len(COLUMN))]
        pltpu.make_async_copy(got, got, meta2_r).wait()
        own_of = jnp.where(iota((NG, 256), 1) // 16 == iota((NG, 256), 0), metas2[:, 0, 0:1], 0.0)
        spread2[...] = (base2[...] * jnp.sum(own_of, axis=0, keepdims=True)).astype(jnp.bfloat16)

    def far_open(p):
        own2[p].wait()
        got = took2.at[pl.ds(0, len(COLUMN) * ROWS), far[p]]
        pltpu.make_async_copy(got, got, a2_r.at[p]).wait()
        part2[:, far[p]] = mm(spread2[...], took2[:, far[p]])
        for dev, pm in flat:
            pltpu.make_async_remote_copy(
                src_ref=part2.at[block(pm), far[p]], dst_ref=gathered2.at[m_at, :, far[p]], send_sem=t2_s.at[p],
                recv_sem=t2_r.at[p], device_id=dev, device_id_type=MESH,
            ).start()
        gathered2[m_at, :, far[p]] = part2[block(m_at), far[p]]

    def far_mix(p):
        got = gathered2.at[pl.ds(0, len(FLAT)), :, far[p]]
        pltpu.make_async_copy(got, got, t2_r.at[p]).wait()
        full2[block(m_at), far[p]] = coded(blend2, jnp.sum(gathered2[:, :, far[p]], axis=0), ztot["c3_16"])
        for dev, _ in flat:
            pltpu.make_async_remote_copy(
                src_ref=full2.at[block(m_at), far[p]], dst_ref=full2.at[block(m_at), far[p]], send_sem=g2_s.at[p],
                recv_sem=g2_r.at[p], device_id=dev, device_id_type=MESH,
            ).start()

    def far_send(p):
        got = full2.at[pl.ds(0, len(FLAT) * ROWS), far[p]]
        pltpu.make_async_copy(got, got, g2_r.at[p]).wait()
        chosen2[:, far[p]] = selected(pick2, full2[:, far[p]])
        for dev, pe in column:
            pltpu.make_async_remote_copy(
                src_ref=chosen2.at[block(pe), far[p]], dst_ref=codes.at[block(e), rest[p]], send_sem=b2_s.at[p],
                recv_sem=b2_r.at[p], device_id=dev, device_id_type=MESH,
            ).start()
        codes[block(e), rest[p]] = chosen2[block(e), far[p]]

    def full_copy(p, owner, dz, role):
        return pltpu.make_async_remote_copy(
            src_ref=full.at[chunk(owner), lanes_of[p]], dst_ref=full.at[chunk(owner), lanes_of[p]],
            send_sem=g_s.at[p, role], recv_sem=g_r.at[p, role], device_id=z_peer(side(p, dz) % NZ), device_id_type=MESH,
        )

    def full_send(p, owner, dz, role):
        cp = full_copy(p, side(p, owner), dz, role)
        cp.start()
        sent.append(cp)

    def full_wait(p, *roles):
        for role in roles:
            full_copy(p, 0, 1, role).wait_recv()

    def mix_piece(p):
        tree_wait(p, 3, 4, 5, 6)
        total = own_part(p, 0)[...]
        for slot in (3, 4, 5, 6):
            total = total + tree[slot, :, lanes_of[p]]
        full[chunk(0), lanes_of[p]] = coded(blend, total, ztot["c3"])
        full_send(p, 0, 2, 2)
        full_send(p, 0, -2, 3)
        full_send(p, 0, 1, 0)
        full_send(p, 0, -1, 1)

    def pass_piece(p):
        full_wait(p, 2)
        full_send(p, -2, 2, 5)
        full_send(p, -2, 1, 4)
        full_wait(p, 3)
        full_send(p, 2, -1, 6)

    def send_piece(p):
        full_wait(p, 0, 1, 4, 5, 6)
        chosen[:, lanes_of[p]] = selected(pick, full[:, lanes_of[p]])
        rs, ls = piece_of(q, p)
        for dev, pq in peers:
            pltpu.make_async_remote_copy(
                src_ref=chosen.at[block(pq), lanes_of[p]], dst_ref=codes.at[rs, ls],
                send_sem=b_s.at[p], recv_sem=b_r.at[p], device_id=dev, device_id_type=MESH,
            ).start()
        codes[rs, ls] = chosen[block(q), lanes_of[p]]

    stages = {
        "open": open_piece, "relay": relay_piece, "mix": mix_piece, "pass": pass_piece, "send": send_piece,
        "totals": lambda p: totals_now(), "far_weights": far_weights, "far_open": far_open, "far_mix": far_mix, "far_send": far_send,
    }
    for name, p in ORDER:
        stages[name](p)

    rows31 = pl.ds(0, len(PLANE) * ROWS)
    for p in range(PIECES):
        got = chosen.at[rows31, lanes_of[p]]
        pltpu.make_async_copy(got, got, b_r.at[p]).wait()
    for p in range(FAR):
        b2 = chosen2.at[pl.ds(0, len(COLUMN) * ROWS), far[p]]
        pltpu.make_async_copy(b2, b2, b2_r.at[p]).wait()
        pltpu.make_async_copy(b2, b2, b2_s.at[p]).wait()
        a2 = took2.at[pl.ds(0, len(COLUMN) * ROWS), far[p]]
        pltpu.make_async_copy(a2, a2, a2_s.at[p]).wait()
        t2 = gathered2.at[pl.ds(0, len(FLAT)), :, far[p]]
        pltpu.make_async_copy(t2, t2, t2_s.at[p]).wait()
        g2 = full2.at[pl.ds(0, len(FLAT) * ROWS), far[p]]
        pltpu.make_async_copy(g2, g2, g2_s.at[p]).wait()
    pltpu.make_async_copy(meta_bytes, meta_bytes, meta_s).wait()
    m2 = metas2.at[pl.ds(0, len(COLUMN))]
    pltpu.make_async_copy(m2, m2, meta2_s).wait()
    zm = zmetas.at[pl.ds(0, NZ - 1)]
    pltpu.make_async_copy(zm, zm, zmeta_s).wait()
    for cp in sent:
        cp.wait_send()
    for p in range(PIECES):
        a = took.at[rows31, lanes_of[p]]
        pltpu.make_async_copy(a, a, a_s.at[p]).wait()
        b = chosen.at[rows31, lanes_of[p]]
        pltpu.make_async_copy(b, b, b_s.at[p]).wait()


def decode(codes, info, averaged, total):
    number = codes[...].astype(jnp.float32)
    size = info[0, 127] * jnp.exp2((jnp.abs(number) - TOP) * (OCTAVES / TOP))
    averaged[...] = jnp.where(number == 0, 0.0, jnp.where(number < 0, -size, size))
    total[...] = info[0:1, 0:1].astype(jnp.int32)


def stay(array):
    return pltpu.with_memory_space_constraint(array, pltpu.HBM)


def local(gradients, token_counts, row_groups, col_groups):
    flat = gradients.reshape(256, 1536)
    dma = pltpu.SemaphoreType.DMA
    vmem = pl.BlockSpec(memory_space=pltpu.VMEM)
    hbm = pl.BlockSpec(memory_space=pltpu.HBM)
    codes, info = pl.pallas_call(
        body,
        out_shape=(
            jax.ShapeDtypeStruct((256, 1536), jnp.int16),
            jax.ShapeDtypeStruct((8, 128), jnp.float32),
        ),
        in_specs=[hbm, pl.BlockSpec(memory_space=pltpu.VMEM), hbm, hbm],
        out_specs=(vmem, vmem),
        scratch_shapes=[
            pltpu.VMEM((256, 1536), jnp.bfloat16),
            pltpu.VMEM((2, NG, NG), jnp.int32),
            pltpu.VMEM((1, NG, NG), jnp.int32),
            pltpu.VMEM((1, 128), jnp.float32),
            pltpu.VMEM((NPLANE, 1, 128), jnp.float32),
            pltpu.VMEM((1, 128), jnp.float32),
            pltpu.VMEM((NZ, 1, 128), jnp.float32),
            pltpu.VMEM((512, LANES), jnp.bfloat16),
            pltpu.VMEM((256, 512), jnp.float32),
            pltpu.VMEM((512, 256), jnp.bfloat16),
            pltpu.VMEM((256, 512), jnp.bfloat16),
            pltpu.VMEM((32, 96), jnp.bfloat16),
            pltpu.VMEM((256, LANES), jnp.float32),
            pltpu.VMEM((7, 32, LANES), jnp.float32),
            pltpu.VMEM((256, LANES), jnp.int16),
            pltpu.VMEM((512, LANES), jnp.int16),
            pltpu.VMEM((NG, 1, 128), jnp.float32),
            pltpu.VMEM((256, REST), jnp.bfloat16),
            pltpu.VMEM((256, 256), jnp.float32),
            pltpu.VMEM((256, 256), jnp.bfloat16),
            pltpu.VMEM((256, 256), jnp.bfloat16),
            pltpu.VMEM((NG, 48), jnp.bfloat16),
            pltpu.VMEM((256, REST), jnp.float32),
            pltpu.VMEM((NG, NG, REST), jnp.float32),
            pltpu.VMEM((256, REST), jnp.int16),
            pltpu.VMEM((256, REST), jnp.int16),
            dma, dma((2,)), dma((PIECES,)), dma, dma, dma, dma,
            dma((PIECES,)), dma((PIECES,)),
            dma((PIECES, 7)), dma((PIECES, 7)), dma((PIECES, 7)), dma((PIECES, 7)),
            dma((PIECES,)), dma((PIECES,)),
            *(dma((FAR,)) for _ in range(9)),
            dma, dma,
        ],
        compiler_params=pltpu.CompilerParams(collective_id=0, has_side_effects=True, vmem_limit_bytes=GRANT),
        name="group_average",
    )(stay(flat), token_counts, stay(row_groups), stay(col_groups))
    averaged, total = pl.pallas_call(
        decode,
        grid=(STEPS,),
        out_shape=(
            jax.ShapeDtypeStruct((256, 1536), jnp.float32),
            jax.ShapeDtypeStruct((1, 1), jnp.int32),
        ),
        in_specs=[
            pl.BlockSpec((256 // STEPS, 1536), lambda s: (s, 0)),
            pl.BlockSpec((8, 128), lambda s: (0, 0)),
        ],
        out_specs=(
            pl.BlockSpec((256 // STEPS, 1536), lambda s: (s, 0)),
            pl.BlockSpec((1, 1), lambda s: (0, 0)),
        ),
        compiler_params=pltpu.CompilerParams(vmem_limit_bytes=GRANT2),
        name="decode",
    )(codes, info)
    return averaged.reshape(gradients.shape), total.reshape(token_counts.shape)


def solution(mesh):
    placed = (P("row", "col", None, None, None), P("row", "col"), P(), P())
    return jax.shard_map(
        local,
        mesh=mesh,
        in_specs=placed,
        out_specs=(P("row", "col", None, None, None), P("row", "col")),
        check_vma=False,
    )
```

```python
import jax
import jax.numpy as jnp
from jax import lax
from jax.experimental import pallas as pl
from jax.experimental.pallas import tpu as pltpu
from jax.sharding import PartitionSpec as P

MESH = pl.DeviceIdType.MESH
NZ = 8
NPLANE = 32
NG = 16
ROWS = 16
WIDTHS = (256, 256)
LANES = sum(WIDTHS)
SPLIT = 2 * LANES
REST = 1536 - SPLIT
FAR = 2
FARW = REST // FAR
PIECES = len(WIDTHS)
STARTS = tuple(sum(WIDTHS[:p]) for p in range(PIECES))
OCTAVES = 24.0
TOP = 32767.0
TINY = 1.2e-38
GRANT = 24 * 1024 * 1024
GRANT2 = 16 * 1024 * 1024
STEPS = 2

ORDER = (("far_weights", 0), ("open", 0), ("open", 1), ("far_open", 0), ("far_open", 1), ("relay", 0), ("relay", 1), ("totals", 0), ("mix", 0), ("mix", 1), ("far_mix", 0), ("far_mix", 1), ("pass", 0), ("pass", 1), ("send", 0), ("far_send", 0), ("far_send", 1), ("send", 1))
PLANE = sorted(
    [(dx, dy, dc) for dx in range(4) for dy in range(4) for dc in range(2) if (dx, dy, dc) != (0, 0, 0)],
    key=lambda off: -(min(off[0], 4 - off[0]) + min(off[1], 4 - off[1])),
)
ZS = (1, 7, 2, 6, 3, 5, 4)
COLUMN = [(dz, dc) for dz in (4, 3, 5, 2, 6, 1, 7, 0) for dc in (0, 1) if (dz, dc) != (0, 0)]
FLAT = [off[:2] for off in PLANE if off[2] == 0]


def iota(shape, dim):
    return lax.broadcasted_iota(jnp.int32, shape, dim)


def onehot(cond):
    return jnp.where(cond, 1.0, 0.0).astype(jnp.bfloat16)


def mm(a, b):
    return jnp.dot(a, b, preferred_element_type=jnp.float32)


def mm_nt(a, b):
    return lax.dot_general(a, b, (((1,), (1,)), ((), ())), preferred_element_type=jnp.float32)


def small(ints):
    return ints.astype(jnp.float32).astype(jnp.bfloat16)


def body(
    grad, count, rg_in, cg_in, codes, info,
    gv, rg, cg, mine, metas, zmine, zmetas, took, base, pick, spread, blend, part, tree, full, chosen,
    metas2, took2, base2, pick2, spread2, blend2, part2, gathered2, full2, chosen2,
    load_sem, small_sem, own_sem, meta_s, meta_r, zmeta_s, zmeta_r, a_s, a_r, t_s, t_r, g_s, g_r, b_s, b_r,
    own2_sem, a2_s, a2_r, t2_s, t2_r, g2_s, g2_r, b2_s, b2_r, meta2_s, meta2_r,
):
    row, col = lax.axis_index("row"), lax.axis_index("col")
    z, xl = row // 2, row % 2
    xh, y, c = col // 8, (col // 2) % 4, col % 2
    x = 2 * xh + xl
    q = xl * 16 + col

    def plane_peer(off):
        px, py, pc = (x + off[0]) % 4, (y + off[1]) % 4, (c + off[2]) % 2
        pcol = ((px // 2) * 4 + py) * 2 + pc
        return (2 * z + px % 2, pcol), (px % 2) * 16 + pcol

    def z_peer(dz):
        return (2 * ((z + dz) % NZ) + xl, col)

    def spot(which):
        return pl.multiple_of((which // 2) * ROWS, ROWS), (which % 2) * LANES

    def piece_of(which, p):
        r0, l0 = spot(which)
        return pl.ds(r0, ROWS), pl.ds(pl.multiple_of(l0 + STARTS[p], 128), WIDTHS[p])

    lanes_of = [pl.ds(STARTS[p], WIDTHS[p]) for p in range(PIECES)]

    def block(which):
        return pl.ds(pl.multiple_of(which * ROWS, ROWS), ROWS)

    def column_peer(off):
        pz, pc = (z + off[0]) % NZ, (c + off[1]) % 2
        return (2 * pz + xl, (xh * 4 + y) * 2 + pc), 2 * pz + pc

    def flat_peer(off):
        px, py = (x + off[0]) % 4, (y + off[1]) % 4
        return (2 * z + px % 2, ((px // 2) * 4 + py) * 2 + c), px * 4 + py

    e, m_at = 2 * z + c, 4 * x + y
    peers = [plane_peer(off) for off in PLANE]
    column = [column_peer(off) for off in COLUMN]
    flat = [flat_peer(off) for off in FLAT]
    others = [peer[0] for off, peer in zip(COLUMN, column) if off[0] and off[1]]
    rest = [pl.ds(SPLIT + p * FARW, FARW) for p in range(FAR)]
    far = [pl.ds(p * FARW, FARW) for p in range(FAR)]

    load = pltpu.make_async_copy(grad, gv, load_sem)
    load.start()
    tables = [
        pltpu.make_async_copy(src, dst, small_sem.at[k])
        for k, (src, dst) in enumerate(((rg_in, rg), (cg_in, cg)))
    ]
    for table in tables:
        table.start()
    own2 = []
    for p in range(FAR):
        own2.append(pltpu.make_async_copy(grad.at[block(e), rest[p]], took2.at[block(e), far[p]], own2_sem.at[p]))
        own2[p].start()
    owns = []
    for p in range(PIECES):
        rs, ls = piece_of(q, p)
        own = pltpu.make_async_copy(grad.at[rs, ls], took.at[block(q), lanes_of[p]], own_sem.at[p])
        own.start()
        owns.append(own)

    barrier = pltpu.get_barrier_semaphore()
    for dev, _ in peers:
        pl.semaphore_signal(barrier, inc=1, device_id=dev, device_id_type=MESH)
    for dz in ZS:
        pl.semaphore_signal(barrier, inc=1, device_id=z_peer(dz), device_id_type=MESH)
    for dev in others:
        pl.semaphore_signal(barrier, inc=1, device_id=dev, device_id_type=MESH)

    load.wait()
    for table in tables:
        table.wait()
    largest = jnp.max(jnp.abs(gv[...].astype(jnp.float32)))
    own_w = count[...].astype(jnp.float32)
    mine[...] = jnp.where(iota((1, 128), 1) < 64, own_w, largest)

    pl.semaphore_wait(barrier, len(PLANE) + len(ZS) + len(others))

    waits = []
    meta_bytes = metas.at[pl.ds(0, len(PLANE))]
    for dev, _ in peers:
        pltpu.make_async_remote_copy(
            src_ref=mine, dst_ref=metas.at[q], send_sem=meta_s, recv_sem=meta_r, device_id=dev, device_id_type=MESH
        ).start()
    for dev, _ in column:
        pltpu.make_async_remote_copy(
            src_ref=mine, dst_ref=metas2.at[e], send_sem=meta2_s, recv_sem=meta2_r, device_id=dev, device_id_type=MESH
        ).start()
    for p in range(max(PIECES, FAR)):
        if p < FAR:
            for dev, pe in column:
                pltpu.make_async_remote_copy(
                    src_ref=gv.at[block(pe), rest[p]], dst_ref=took2.at[block(e), far[p]], send_sem=a2_s.at[p],
                    recv_sem=a2_r.at[p], device_id=dev, device_id_type=MESH,
                ).start()
        if p < PIECES:
            for dev, pq in peers:
                rs, ls = piece_of(pq, p)
                pltpu.make_async_remote_copy(
                    src_ref=gv.at[rs, ls], dst_ref=took.at[block(q), lanes_of[p]],
                    send_sem=a_s.at[p], recv_sem=a_r.at[p], device_id=dev, device_id_type=MESH,
                ).start()
    metas[q] = mine[...]
    metas2[e] = mine[...]

    rg0, rg1, cg0 = small(rg[0]), small(rg[1]), small(cg[0])
    eye = onehot(iota((NG, NG), 0) == iota((NG, NG), 1))
    by_i = onehot(iota((256, NG), 0) // 16 == iota((256, NG), 1))
    j_of = (iota((256, NG), 0) % 16).astype(jnp.float32)
    first = onehot(mm(by_i, rg0) == j_of)
    last = onehot(mm(by_i, rg1) == j_of)
    n_i = onehot(iota((NG, 256), 1) // 16 == iota((NG, 256), 0))
    n_j = onehot(iota((NG, 256), 1) % 16 == iota((NG, 256), 0))
    cols_t = mm_nt(eye, cg0).astype(jnp.bfloat16)
    rows_t = mm_nt(eye, rg1).astype(jnp.bfloat16)
    middle = onehot(mm(cols_t, n_j) == (iota((NG, 256), 1) // 16).astype(jnp.float32))
    third = onehot(mm(rows_t, n_i) == (iota((NG, 256), 1) % 16).astype(jnp.float32))
    m2 = mm(middle, first).astype(jnp.bfloat16)
    m3 = mm_nt(third, middle).astype(jnp.bfloat16)
    m = mm(m3, m2)
    mb = m.astype(jnp.bfloat16)

    in_plane = onehot(iota((NPLANE, 256), 1) == iota((NPLANE, 256), 0) + 32 * z)
    first_z = mm(in_plane, first).astype(jnp.bfloat16)
    last_z = mm(in_plane, last).astype(jnp.bfloat16)
    row_g = onehot(iota((256, NG), 0) % 16 == iota((256, NG), 1))
    col_q = onehot(iota((NPLANE, 512), 1) // 16 == iota((NPLANE, 512), 0))
    wide = mm(mm_nt(row_g, first_z).astype(jnp.bfloat16), col_q)
    base[...] = jnp.where(iota((256, 512), 0) // 16 == iota((256, 512), 1) % 16, wide, 0.0)
    row_q = onehot(iota((512, NPLANE), 0) // 16 == iota((512, NPLANE), 1))
    col_k = onehot(iota((NG, 256), 1) % 16 == iota((NG, 256), 0))
    tall = mm(mm(row_q, last_z).astype(jnp.bfloat16), col_k)
    pick[...] = jnp.where(iota((512, 256), 0) % 16 == iota((512, 256), 1) // 16, tall, 0.0).astype(jnp.bfloat16)

    r32 = onehot(iota((32, NG), 0) % 16 == iota((32, NG), 1))
    c96 = onehot(iota((NG, 96), 1) % 16 == iota((NG, 96), 0))
    mix = mm(mm(r32, mb).astype(jnp.bfloat16), c96)
    blend[...] = jnp.where(iota((32, 96), 0) // 16 == (iota((32, 96), 1) // 16) % 2, mix, 0.0).astype(jnp.bfloat16)

    n_e = 32 * (iota((NG, 256), 0) // 2) + xl * 16 + (xh * 4 + y) * 2 + iota((NG, 256), 0) % 2
    in_column = onehot(iota((NG, 256), 1) == n_e)
    first_e = mm(in_column, first).astype(jnp.bfloat16)
    last_e = mm(in_column, last).astype(jnp.bfloat16)
    wide2 = mm(mm_nt(row_g, first_e).astype(jnp.bfloat16), n_i)
    base2[...] = jnp.where(iota((256, 256), 0) // 16 == iota((256, 256), 1) % 16, wide2, 0.0)
    tall2 = mm(mm(by_i, last_e).astype(jnp.bfloat16), col_k)
    pick2[...] = jnp.where(iota((256, 256), 0) % 16 == iota((256, 256), 1) // 16, tall2, 0.0).astype(jnp.bfloat16)
    blend2[...] = mm(mb, onehot(iota((NG, 48), 1) % 16 == iota((NG, 48), 0))).astype(jnp.bfloat16)

    pltpu.make_async_copy(meta_bytes, meta_bytes, meta_r).wait()
    held = metas[:, 0, :]
    lane = iota((NPLANE, 128), 1)
    plane_w = jnp.sum(jnp.where(lane == iota((NPLANE, 128), 0), held[:, 0:1], 0.0), axis=0, keepdims=True)
    plane_x = jnp.max(jnp.where(lane >= 64, held, 0.0))
    zmine[...] = jnp.where(iota((1, 128), 1) < NPLANE, plane_w, plane_x)
    for dz in ZS:
        pltpu.make_async_remote_copy(
            src_ref=zmine, dst_ref=zmetas.at[z], send_sem=zmeta_s, recv_sem=zmeta_r, device_id=z_peer(dz), device_id_type=MESH
        ).start()
    zmetas[z] = zmine[...]
    w512 = mm(plane_w[:, 0:NPLANE].astype(jnp.bfloat16), col_q)
    spread[...] = (base[...] * w512).astype(jnp.bfloat16)

    def chunk(dz):
        return pl.ds(pl.multiple_of(((z + dz) % NZ) * 32, 32), 32)

    def side(p, dz):
        return dz if p % 2 == 0 else -dz

    sent = []

    def tree_copy(p, src, dz, slot):
        return pltpu.make_async_remote_copy(
            src_ref=src, dst_ref=tree.at[slot, :, lanes_of[p]], send_sem=t_s.at[p, slot], recv_sem=t_r.at[p, slot],
            device_id=z_peer(side(p, dz) % NZ), device_id_type=MESH,
        )

    def tree_send(p, src, dz, slot):
        cp = tree_copy(p, src, dz, slot)
        cp.start()
        sent.append(cp)

    def tree_wait(p, *slots):
        for slot in slots:
            tree_copy(p, part.at[chunk(0), lanes_of[p]], 1, slot).wait_recv()

    def own_part(p, dz):
        return part.at[chunk(side(p, dz)), lanes_of[p]]

    def open_piece(p):
        owns[p].wait()
        got = took.at[pl.ds(0, len(PLANE) * ROWS), lanes_of[p]]
        pltpu.make_async_copy(got, got, a_r.at[p]).wait()
        part[:, lanes_of[p]] = mm(spread[...], took[:, lanes_of[p]])
        tree_send(p, own_part(p, -4), -2, 2)
        tree_send(p, own_part(p, 3), 1, 0)
        tree_send(p, own_part(p, -3), -1, 1)
        tree_send(p, own_part(p, 1), 1, 3)
        tree_send(p, own_part(p, -1), -1, 4)

    def relay_piece(p):
        tree_wait(p, 0)
        tree[0, :, lanes_of[p]] = tree[0, :, lanes_of[p]] + own_part(p, 2)[...]
        tree_send(p, tree.at[0, :, lanes_of[p]], 2, 5)
        tree_wait(p, 1, 2)
        tree[1, :, lanes_of[p]] = tree[1, :, lanes_of[p]] + tree[2, :, lanes_of[p]] + own_part(p, -2)[...]
        tree_send(p, tree.at[1, :, lanes_of[p]], -2, 6)

    ztot = {}

    def totals_now():
        got = zmetas.at[pl.ds(0, NZ - 1)]
        pltpu.make_async_copy(got, got, zmeta_r).wait()
        cw = zmetas[:, 0, :]
        by_z = onehot(iota((256, NZ), 0) // 32 == iota((256, NZ), 1))
        lanes = iota((256, 128), 1)
        all_x = jnp.maximum(jnp.max(jnp.where(iota((NZ, 128), 1) >= NPLANE, cw, 0.0)), TINY)
        counts = jnp.where(iota((NZ, 128), 1) < NPLANE, cw, 0.0).astype(jnp.bfloat16)
        spread_w = mm(by_z, counts)
        w_col = jnp.sum(jnp.where(lanes == iota((256, 128), 0) % 32, spread_w, 0.0), axis=1, keepdims=True)
        c1 = jnp.sum(first.astype(jnp.float32) * w_col, axis=0, keepdims=True)
        c3 = jnp.sum(m * c1, axis=1, keepdims=True)
        ztot["x"] = all_x
        ztot["c3_16"] = c3
        ztot["c3"] = jnp.concatenate([c3, c3], axis=0)
        is_me = onehot(iota((NG, NPLANE), 1) == q)
        mine_k = mm(is_me, last_z)
        own_c3 = jnp.sum(jnp.where(iota((NG, NG), 0) == iota((NG, NG), 1), mine_k, 0.0) * c3)
        info[...] = jnp.where(iota((8, 128), 1) < 64, own_c3, all_x)

    def coded(mixing, total, weights):
        hi = total.astype(jnp.bfloat16)
        after = total - hi.astype(jnp.float32)
        mid = after.astype(jnp.bfloat16)
        low = (after - mid.astype(jnp.float32)).astype(jnp.bfloat16)
        avg = mm(mixing[...], jnp.concatenate([hi, mid, low], axis=0)) / weights
        size = jnp.abs(avg) * (1.0 / ztot["x"])
        level = TOP + jnp.log2(jnp.maximum(size, 1e-30)) * (TOP / OCTAVES)
        level = jnp.clip(jnp.round(level), 0.0, TOP)
        return jnp.where(avg < 0, -level, level).astype(jnp.int32).astype(jnp.int16)

    def selected(picking, values):
        code = values.astype(jnp.int32)
        high = mm(picking[...], small(code >> 8))
        lows = mm(picking[...], small(code & 255))
        return (high * 256.0 + lows).astype(jnp.int32).astype(jnp.int16)

    def far_weights(p):
        got = metas2.at[pl.ds(0, len(COLUMN))]
        pltpu.make_async_copy(got, got, meta2_r).wait()
        own_of = jnp.where(iota((NG, 256), 1) // 16 == iota((NG, 256), 0), metas2[:, 0, 0:1], 0.0)
        spread2[...] = (base2[...] * jnp.sum(own_of, axis=0, keepdims=True)).astype(jnp.bfloat16)

    def far_open(p):
        own2[p].wait()
        got = took2.at[pl.ds(0, len(COLUMN) * ROWS), far[p]]
        pltpu.make_async_copy(got, got, a2_r.at[p]).wait()
        part2[:, far[p]] = mm(spread2[...], took2[:, far[p]])
        for dev, pm in flat:
            pltpu.make_async_remote_copy(
                src_ref=part2.at[block(pm), far[p]], dst_ref=gathered2.at[m_at, :, far[p]], send_sem=t2_s.at[p],
                recv_sem=t2_r.at[p], device_id=dev, device_id_type=MESH,
            ).start()
        gathered2[m_at, :, far[p]] = part2[block(m_at), far[p]]

    def far_mix(p):
        got = gathered2.at[pl.ds(0, len(FLAT)), :, far[p]]
        pltpu.make_async_copy(got, got, t2_r.at[p]).wait()
        full2[block(m_at), far[p]] = coded(blend2, jnp.sum(gathered2[:, :, far[p]], axis=0), ztot["c3_16"])
        for dev, _ in flat:
            pltpu.make_async_remote_copy(
                src_ref=full2.at[block(m_at), far[p]], dst_ref=full2.at[block(m_at), far[p]], send_sem=g2_s.at[p],
                recv_sem=g2_r.at[p], device_id=dev, device_id_type=MESH,
            ).start()

    def far_send(p):
        got = full2.at[pl.ds(0, len(FLAT) * ROWS), far[p]]
        pltpu.make_async_copy(got, got, g2_r.at[p]).wait()
        chosen2[:, far[p]] = selected(pick2, full2[:, far[p]])
        for dev, pe in column:
            pltpu.make_async_remote_copy(
                src_ref=chosen2.at[block(pe), far[p]], dst_ref=codes.at[block(e), rest[p]], send_sem=b2_s.at[p],
                recv_sem=b2_r.at[p], device_id=dev, device_id_type=MESH,
            ).start()
        codes[block(e), rest[p]] = chosen2[block(e), far[p]]

    def full_copy(p, owner, dz, role):
        return pltpu.make_async_remote_copy(
            src_ref=full.at[chunk(owner), lanes_of[p]], dst_ref=full.at[chunk(owner), lanes_of[p]],
            send_sem=g_s.at[p, role], recv_sem=g_r.at[p, role], device_id=z_peer(side(p, dz) % NZ), device_id_type=MESH,
        )

    def full_send(p, owner, dz, role):
        cp = full_copy(p, side(p, owner), dz, role)
        cp.start()
        sent.append(cp)

    def full_wait(p, *roles):
        for role in roles:
            full_copy(p, 0, 1, role).wait_recv()

    def mix_piece(p):
        tree_wait(p, 3, 4, 5, 6)
        total = own_part(p, 0)[...]
        for slot in (3, 4, 5, 6):
            total = total + tree[slot, :, lanes_of[p]]
        full[chunk(0), lanes_of[p]] = coded(blend, total, ztot["c3"])
        full_send(p, 0, 2, 2)
        full_send(p, 0, -2, 3)
        full_send(p, 0, 1, 0)
        full_send(p, 0, -1, 1)

    def pass_piece(p):
        full_wait(p, 2)
        full_send(p, -2, 2, 5)
        full_send(p, -2, 1, 4)
        full_wait(p, 3)
        full_send(p, 2, -1, 6)

    def send_piece(p):
        full_wait(p, 0, 1, 4, 5, 6)
        chosen[:, lanes_of[p]] = selected(pick, full[:, lanes_of[p]])
        rs, ls = piece_of(q, p)
        for dev, pq in peers:
            pltpu.make_async_remote_copy(
                src_ref=chosen.at[block(pq), lanes_of[p]], dst_ref=codes.at[rs, ls],
                send_sem=b_s.at[p], recv_sem=b_r.at[p], device_id=dev, device_id_type=MESH,
            ).start()
        codes[rs, ls] = chosen[block(q), lanes_of[p]]

    stages = {
        "open": open_piece, "relay": relay_piece, "mix": mix_piece, "pass": pass_piece, "send": send_piece,
        "totals": lambda p: totals_now(), "far_weights": far_weights, "far_open": far_open, "far_mix": far_mix, "far_send": far_send,
    }
    for name, p in ORDER:
        stages[name](p)

    rows31 = pl.ds(0, len(PLANE) * ROWS)
    for p in range(PIECES):
        got = chosen.at[rows31, lanes_of[p]]
        pltpu.make_async_copy(got, got, b_r.at[p]).wait()
    for p in range(FAR):
        b2 = chosen2.at[pl.ds(0, len(COLUMN) * ROWS), far[p]]
        pltpu.make_async_copy(b2, b2, b2_r.at[p]).wait()
        pltpu.make_async_copy(b2, b2, b2_s.at[p]).wait()
        a2 = took2.at[pl.ds(0, len(COLUMN) * ROWS), far[p]]
        pltpu.make_async_copy(a2, a2, a2_s.at[p]).wait()
        t2 = gathered2.at[pl.ds(0, len(FLAT)), :, far[p]]
        pltpu.make_async_copy(t2, t2, t2_s.at[p]).wait()
        g2 = full2.at[pl.ds(0, len(FLAT) * ROWS), far[p]]
        pltpu.make_async_copy(g2, g2, g2_s.at[p]).wait()
    pltpu.make_async_copy(meta_bytes, meta_bytes, meta_s).wait()
    m2 = metas2.at[pl.ds(0, len(COLUMN))]
    pltpu.make_async_copy(m2, m2, meta2_s).wait()
    zm = zmetas.at[pl.ds(0, NZ - 1)]
    pltpu.make_async_copy(zm, zm, zmeta_s).wait()
    for cp in sent:
        cp.wait_send()
    for p in range(PIECES):
        a = took.at[rows31, lanes_of[p]]
        pltpu.make_async_copy(a, a, a_s.at[p]).wait()
        b = chosen.at[rows31, lanes_of[p]]
        pltpu.make_async_copy(b, b, b_s.at[p]).wait()


def decode(codes, info, averaged, total):
    number = codes[...].astype(jnp.float32)
    size = info[0, 127] * jnp.exp2((jnp.abs(number) - TOP) * (OCTAVES / TOP))
    averaged[...] = jnp.where(number == 0, 0.0, jnp.where(number < 0, -size, size))
    total[...] = info[0:1, 0:1].astype(jnp.int32)


def stay(array):
    return pltpu.with_memory_space_constraint(array, pltpu.HBM)


def local(gradients, token_counts, row_groups, col_groups):
    flat = gradients.reshape(256, 1536)
    dma = pltpu.SemaphoreType.DMA
    vmem = pl.BlockSpec(memory_space=pltpu.VMEM)
    hbm = pl.BlockSpec(memory_space=pltpu.HBM)
    codes, info = pl.pallas_call(
        body,
        out_shape=(
            jax.ShapeDtypeStruct((256, 1536), jnp.int16),
            jax.ShapeDtypeStruct((8, 128), jnp.float32),
        ),
        in_specs=[hbm, pl.BlockSpec(memory_space=pltpu.VMEM), hbm, hbm],
        out_specs=(vmem, vmem),
        scratch_shapes=[
            pltpu.VMEM((256, 1536), jnp.bfloat16),
            pltpu.VMEM((2, NG, NG), jnp.int32),
            pltpu.VMEM((1, NG, NG), jnp.int32),
            pltpu.VMEM((1, 128), jnp.float32),
            pltpu.VMEM((NPLANE, 1, 128), jnp.float32),
            pltpu.VMEM((1, 128), jnp.float32),
            pltpu.VMEM((NZ, 1, 128), jnp.float32),
            pltpu.VMEM((512, LANES), jnp.bfloat16),
            pltpu.VMEM((256, 512), jnp.float32),
            pltpu.VMEM((512, 256), jnp.bfloat16),
            pltpu.VMEM((256, 512), jnp.bfloat16),
            pltpu.VMEM((32, 96), jnp.bfloat16),
            pltpu.VMEM((256, LANES), jnp.float32),
            pltpu.VMEM((7, 32, LANES), jnp.float32),
            pltpu.VMEM((256, LANES), jnp.int16),
            pltpu.VMEM((512, LANES), jnp.int16),
            pltpu.VMEM((NG, 1, 128), jnp.float32),
            pltpu.VMEM((256, REST), jnp.bfloat16),
            pltpu.VMEM((256, 256), jnp.float32),
            pltpu.VMEM((256, 256), jnp.bfloat16),
            pltpu.VMEM((256, 256), jnp.bfloat16),
            pltpu.VMEM((NG, 48), jnp.bfloat16),
            pltpu.VMEM((256, REST), jnp.float32),
            pltpu.VMEM((NG, NG, REST), jnp.float32),
            pltpu.VMEM((256, REST), jnp.int16),
            pltpu.VMEM((256, REST), jnp.int16),
            dma, dma((2,)), dma((PIECES,)), dma, dma, dma, dma,
            dma((PIECES,)), dma((PIECES,)),
            dma((PIECES, 7)), dma((PIECES, 7)), dma((PIECES, 7)), dma((PIECES, 7)),
            dma((PIECES,)), dma((PIECES,)),
            *(dma((FAR,)) for _ in range(9)),
            dma, dma,
        ],
        compiler_params=pltpu.CompilerParams(collective_id=0, has_side_effects=True, vmem_limit_bytes=GRANT),
        name="group_average",
    )(stay(flat), token_counts, stay(row_groups), stay(col_groups))
    averaged, total = pl.pallas_call(
        decode,
        grid=(STEPS,),
        out_shape=(
            jax.ShapeDtypeStruct((256, 1536), jnp.float32),
            jax.ShapeDtypeStruct((1, 1), jnp.int32),
        ),
        in_specs=[
            pl.BlockSpec((256 // STEPS, 1536), lambda s: (s, 0)),
            pl.BlockSpec((8, 128), lambda s: (0, 0)),
        ],
        out_specs=(
            pl.BlockSpec((256 // STEPS, 1536), lambda s: (s, 0)),
            pl.BlockSpec((1, 1), lambda s: (0, 0)),
        ),
        compiler_params=pltpu.CompilerParams(vmem_limit_bytes=GRANT2),
        name="decode",
    )(codes, info)
    return averaged.reshape(gradients.shape), total.reshape(token_counts.shape)


def solution(mesh):
    placed = (P("row", "col", None, None, None), P("row", "col"), P(), P())
    return jax.shard_map(
        local,
        mesh=mesh,
        in_specs=placed,
        out_specs=(P("row", "col", None, None, None), P("row", "col")),
        check_vma=False,
    )
```
